128 devices in a mesh: ta: 4 (over x), gz: 8 (over y, core), xy: 4 (over z).
Axes of the slice: x: 4, y: 4, z: 4, core: 2. Of those that a mesh axis runs over, the one named last changes fastest.
Arguments:
- source: float32 [2, 4, 3, 16, 64, 512], P(None, None, None, 'ta', 'gz', 'xy'), may hold values from -6 to 6
- iterate: float32 [2, 4, 3, 16, 64, 512], P(None, None, None, 'ta', 'gz', 'xy'), may hold values from -6 to 6
- gauge_links: float32 [4, 2, 3, 3, 16, 64, 512], P(None, None, None, None, 'ta', 'gz', 'xy'), may hold values from -2.4 to 2.4
- clover: float32 [2, 2, 6, 6, 16, 64, 512], P(None, None, None, None, 'ta', 'gz', 'xy'), may hold values from -0.6 to 0.6
- bc_sign: int32 [4], replicated, may hold values from -1 to 1, as said below
- null_store: bfloat16 [4, 16, 4, 2, 24, 12, 4, 4, 128], P('ta', 'gz', 'xy'), may hold values from -0.109375 to 0.109375
- block_slot: int32 [4, 16, 4], P('ta', 'gz', 'xy'), may hold values from 0 to 1, as said below
- coarse_links: float32 [9, 2, 24, 24, 4, 16, 4, 8], P(None, None, None, None, 'ta', 'gz', 'xy'), may hold values from -0.2 to 0.2
Outputs:
- new_iterate: float32 [2, 4, 3, 16, 64, 512], P(None, None, None, 'ta', 'gz', 'xy')
- new_residual: float32 [2, 4, 3, 16, 64, 512], P(None, None, None, 'ta', 'gz', 'xy')
The draws below stay inside these ranges and needn't reach their ends.
Inputs may be any that keep to these rules, and one draw needn't show every extreme that they name: `bc_sign`: each entry is -1 or +1. `block_slot`: within each device's block of 2 aggregate columns the entries are the numbers 0 to 1, each once.
All inputs are finite; a program needn't handle non-finite values.
Results may differ from the reference program's by a relative error of at most 0.0016.
Values sent between devices are 32-bit elements; how exact they have to be, the bound alone decides.
A program may use at most 256 MiB of HBM per device.

```python
import jax
import jax.numpy as jnp
import numpy as np
from jax import lax

NV = 24
BLK = 4
LT = 4
LZ = 8
LX = 4
LY = 32
CITERS = 4
NT = 16
NZ = 64
NXY = 512
CT = 4
CZ = 16
CX = 4
CY = 8


def draw_bc_sign(key, part):
    return 2 * jax.random.randint(key, (4,), 0, 2, dtype=jnp.int32) - 1


def draw_block_slot(key, part):
    dev_t = LT // BLK
    dev_z = LZ // BLK
    dev_x = LX // BLK
    count_t = CT // dev_t
    count_z = CZ // dev_z
    count_x = CX // dev_x
    per_device = dev_t * dev_z * dev_x
    scores = jax.random.randint(key, (count_t * count_z * count_x, per_device), 0, 1 << 16, dtype=jnp.int32)
    scores = scores * per_device + jnp.arange(per_device, dtype=jnp.int32)[None, :]
    ordering = jnp.argsort(scores, axis=1).astype(jnp.int32)
    ordering = ordering.reshape((count_t, count_z, count_x, dev_t, dev_z, dev_x))
    ordering = jnp.transpose(ordering, (0, 3, 1, 4, 2, 5))
    return ordering.reshape((CT, CZ, CX))


def level_of(own_key, shape, split, smallest, high):
    def one(dim, parts):
        draws = jax.random.uniform(jax.random.fold_in(jax.random.fold_in(own_key, 6), dim), (parts,), jnp.float32, smallest / len(split), high / len(split))
        return jnp.repeat(jnp.exp(draws), shape[dim] // parts).reshape((-1,) + (1,) * (len(shape) - dim - 1))

    loudness = one(*split[0])
    for cut in split[1:]:
        loudness = loudness * one(*cut)
    return loudness


def scatter_about(stream_key, shape, scale, bound, cuts=(), kind=jnp.bfloat16):
    values = scale * jax.random.normal(stream_key, shape, jnp.float32)
    if cuts:
        values = values * level_of(stream_key, shape, cuts, -0.22, 0.18)
    return jnp.clip(values, -bound, bound).astype(kind)


def setup_inputs(seed: int = 0) -> dict:
    key_list = jax.random.split(jax.random.key(seed), 9)
    source = scatter_about(key_list[0], (2, 4, 3, NT, NZ, NXY), 1.0, 6.0, ((3, 4), (4, 8), (5, 4)), jnp.float32)
    iterate = scatter_about(key_list[1], (2, 4, 3, NT, NZ, NXY), 1.0, 6.0, ((3, 4), (4, 8), (5, 4)), jnp.float32)
    gauge_links = scatter_about(key_list[2], (4, 2, 3, 3, NT, NZ, NXY), 0.4, 2.4, ((4, 4), (5, 8), (6, 4)), jnp.float32)
    clover = scatter_about(key_list[3], (2, 2, 6, 6, NT, NZ, NXY), 0.1, 0.6, ((4, 4), (5, 8), (6, 4)), jnp.float32)
    bc_sign = draw_bc_sign(jax.random.fold_in(key_list[8], 71), 0)
    null_store = scatter_about(key_list[5], (CT, CZ, CX, 2, NV, 12, BLK, BLK, BLK * LY), (12 * BLK ** 4) ** -0.5, 0.109375, ((0, 4), (1, 8), (2, 4)))
    block_slot = draw_block_slot(jax.random.fold_in(key_list[8], 71), 0)
    coarse_links = scatter_about(key_list[7], (9, 2, NV, NV, CT, CZ, CX, CY), 0.03, 0.2, ((4, 4), (5, 8), (6, 4)), jnp.float32)
    return {"source": source, "iterate": iterate, "gauge_links": gauge_links, "clover": clover, "bc_sign": bc_sign, "null_store": null_store, "block_slot": block_slot, "coarse_links": coarse_links}


MASS_TERM = 3.8
RELAX_WEIGHT = 0.4
HIGHEST = lax.Precision.HIGHEST


def chiral_blocks():
    identity = np.eye(2)
    nought = np.zeros((2, 2))
    flip_x = np.array([[0.0, 1.0], [1.0, 0.0]])
    flip_z = np.array([[1.0, 0.0], [0.0, -1.0]])
    rotate = np.array([[0.0, -1.0], [1.0, 0.0]])
    return [(identity, nought), (nought, -flip_z), (nought, -flip_x), (rotate, nought)]


def four_square(top_left, top_right, bottom_left, bottom_right):
    upper = np.concatenate([top_left, top_right], axis=1)
    lower = np.concatenate([bottom_left, bottom_right], axis=1)
    return np.concatenate([upper, lower], axis=0)


def spin_tables(direction, parity):
    upper_re, upper_im = chiral_blocks()[direction]
    identity = np.eye(2)
    nought = np.zeros((2, 2))
    gamma_re = four_square(nought, upper_re, upper_re.T, nought)
    gamma_im = four_square(nought, upper_im, -upper_im.T, nought)
    whole_re = np.eye(4) + parity * gamma_re
    whole_im = parity * gamma_im
    half_re = np.concatenate([identity, parity * upper_re], axis=1)
    half_im = np.concatenate([nought, parity * upper_im], axis=1)
    back_re = np.concatenate([identity, parity * upper_re.T], axis=0)
    back_im = np.concatenate([nought, -parity * upper_im.T], axis=0)
    return [np.asarray(matrix, np.float32) for matrix in (whole_re, whole_im, half_re, half_im, back_re, back_im)]


def spin_times(matrix_re, matrix_im, field):
    real_part = jnp.tensordot(matrix_re, field[0], axes=(1, 0), precision=HIGHEST) - jnp.tensordot(matrix_im, field[1], axes=(1, 0), precision=HIGHEST)
    imag_part = jnp.tensordot(matrix_re, field[1], axes=(1, 0), precision=HIGHEST) + jnp.tensordot(matrix_im, field[0], axes=(1, 0), precision=HIGHEST)
    return jnp.stack([real_part, imag_part])


def colour_times(link, field):
    real_part = 0.0
    imag_part = 0.0
    for column in range(3):
        link_re = link[0][:, column][None]
        link_im = link[1][:, column][None]
        field_re = field[0][:, column:column + 1]
        field_im = field[1][:, column:column + 1]
        real_part = real_part + link_re * field_re - link_im * field_im
        imag_part = imag_part + link_re * field_im + link_im * field_re
    return jnp.stack([real_part, imag_part])


def colour_dagger(link, field):
    real_part = 0.0
    imag_part = 0.0
    for column in range(3):
        link_re = link[0][column][None]
        link_im = link[1][column][None]
        field_re = field[0][:, column:column + 1]
        field_im = field[1][:, column:column + 1]
        real_part = real_part + link_re * field_re + link_im * field_im
        imag_part = imag_part + link_re * field_im - link_im * field_re
    return jnp.stack([real_part, imag_part])


def clover_times(clover, field):
    halves = []
    for chirality in range(2):
        chiral_part = field[:, 2 * chirality:2 * chirality + 2]
        chiral_part = chiral_part.reshape((2, 6) + chiral_part.shape[3:])
        matrix_re = clover[chirality, 0]
        matrix_im = clover[chirality, 1]
        real_part = 0.0
        imag_part = 0.0
        for column in range(6):
            real_part = real_part + matrix_re[:, column] * chiral_part[0, column][None] - matrix_im[:, column] * chiral_part[1, column][None]
            imag_part = imag_part + matrix_re[:, column] * chiral_part[1, column][None] + matrix_im[:, column] * chiral_part[0, column][None]
        halves.append(jnp.stack([real_part, imag_part]).reshape((2, 2, 3) + chiral_part.shape[2:]))
    return jnp.concatenate(halves, axis=1)


def along_y(field, forward):
    column_y = jnp.arange(field.shape[-1], dtype=jnp.int32) % LY
    if forward:
        return jnp.where(column_y == LY - 1, jnp.roll(field, LY - 1, axis=-1), jnp.roll(field, -1, axis=-1))
    return jnp.where(column_y == 0, jnp.roll(field, 1 - LY, axis=-1), jnp.roll(field, 1, axis=-1))


def neighbour(field, direction, forward):
    offset = -1 if forward else 1
    if direction == 0:
        return jnp.roll(field, offset, axis=-3)
    if direction == 1:
        return jnp.roll(field, offset, axis=-2)
    if direction == 2:
        return jnp.roll(field, offset * LY, axis=-1)
    return along_y(field, forward)


def edge_factors(bc_sign, shape):
    count_t, count_z, count_xy = shape
    flat_index = jnp.arange(count_xy, dtype=jnp.int32)
    places = [(jnp.arange(count_t, dtype=jnp.int32)[:, None, None], count_t),
              (jnp.arange(count_z, dtype=jnp.int32)[None, :, None], count_z),
              ((flat_index // LY)[None, None, :], count_xy // LY),
              ((flat_index % LY)[None, None, :], LY)]
    factors = []
    for direction in range(4):
        where_now, extent = places[direction]
        flipped = bc_sign[direction].astype(jnp.float32)
        factors.append((jnp.where(where_now == extent - 1, flipped, 1.0), jnp.where(where_now == 0, flipped, 1.0)))
    return factors


def fine_apply(field, gauge_links, clover, factors):
    result = MASS_TERM * field + clover_times(clover, field)
    for direction in range(4):
        minus_tables = spin_tables(direction, -1)
        plus_tables = spin_tables(direction, 1)
        ahead = colour_times(gauge_links[direction], neighbour(field, direction, True) * factors[direction][0])
        behind = colour_dagger(neighbour(gauge_links[direction], direction, False), neighbour(field, direction, False) * factors[direction][1])
        result = result - 0.5 * (spin_times(minus_tables[0], minus_tables[1], ahead) + spin_times(plus_tables[0], plus_tables[1], behind))
    return result


def source_index(block_slot):
    dev_t, dev_z, dev_x = LT // BLK, LZ // BLK, LX // BLK
    count_t, count_z, count_x = block_slot.shape
    base_t = jnp.arange(count_t, dtype=jnp.int32)[:, None, None] // dev_t * dev_t
    base_z = jnp.arange(count_z, dtype=jnp.int32)[None, :, None] // dev_z * dev_z
    base_x = jnp.arange(count_x, dtype=jnp.int32)[None, None, :] // dev_x * dev_x
    slot_t = block_slot // (dev_z * dev_x)
    slot_z = block_slot // dev_x % dev_z
    slot_x = block_slot % dev_x
    return (((base_t + slot_t) * count_z + base_z + slot_z) * count_x + base_x + slot_x).astype(jnp.int32)


def column_layout(field):
    width = BLK * LY
    shaped = field.reshape((2, 12, CT, BLK, CZ, BLK, CX, width))
    return jnp.moveaxis(shaped, 2, 0)


def restrict_all(rounded, null_store, indices):
    columns = column_layout(rounded)
    flat_store = null_store.reshape((-1,) + null_store.shape[3:])

    def one_slice(inputs):
        field_part, index_part = inputs
        null_rows = jnp.take(flat_store, index_part.reshape(-1), axis=0).astype(jnp.float32)
        null_rows = null_rows.reshape((CZ, CX) + null_rows.shape[1:])
        field_part = field_part.astype(jnp.float32)
        turned = jnp.stack([field_part[1], -field_part[0]])
        paired = jnp.stack([field_part, turned])
        return jnp.einsum('zxpvsabw,qpsazbxw->qvzxw', null_rows, paired, precision=HIGHEST)

    coarse = lax.map(one_slice, (columns, indices))
    coarse = coarse.reshape(coarse.shape[:5] + (BLK, CY, BLK)).sum(axis=(5, 7))
    return jnp.transpose(coarse, (1, 2, 0, 3, 4, 5))


def prolong_all(coarse_round, null_store, indices):
    width = BLK * LY
    per_slice = jnp.moveaxis(coarse_round, 2, 0)
    flat_store = null_store.reshape((-1,) + null_store.shape[3:])

    def one_slice(inputs):
        coarse_part, index_part = inputs
        null_rows = jnp.take(flat_store, index_part.reshape(-1), axis=0).astype(jnp.float32)
        null_rows = null_rows.reshape((CZ, CX) + null_rows.shape[1:])
        coarse_part = coarse_part.astype(jnp.float32)
        spread = jnp.broadcast_to(coarse_part[..., None, :, None], coarse_part.shape[:4] + (BLK, CY, BLK))
        spread = spread.reshape(coarse_part.shape[:4] + (width,))
        mixture = jnp.stack([jnp.stack([spread[0], -spread[1]]), jnp.stack([spread[1], spread[0]])])
        return jnp.einsum('zxpvsabw,qpvzxw->qsazbxw', null_rows, mixture, precision=HIGHEST)

    fine = lax.map(one_slice, (per_slice, indices))
    fine = jnp.moveaxis(fine, 0, 2)
    return fine.reshape((2, 4, 3, CT * BLK, CZ * BLK, CX * width))


def block_times(block_links, stacked):
    links_re = block_links[:, 0]
    links_im = block_links[:, 1]
    vector_re = stacked[:, 0]
    vector_im = stacked[:, 1]
    real_part = jnp.einsum('kijabcd,kjabcd->iabcd', links_re, vector_re, precision=HIGHEST) - jnp.einsum('kijabcd,kjabcd->iabcd', links_im, vector_im, precision=HIGHEST)
    imag_part = jnp.einsum('kijabcd,kjabcd->iabcd', links_re, vector_im, precision=HIGHEST) + jnp.einsum('kijabcd,kjabcd->iabcd', links_im, vector_re, precision=HIGHEST)
    return jnp.stack([real_part, imag_part])


def coarse_apply(vector, coarse_links):
    neighbours = [vector,
                  jnp.roll(vector, -1, 2), jnp.roll(vector, 1, 2),
                  jnp.roll(vector, -1, 3), jnp.roll(vector, 1, 3),
                  jnp.roll(vector, -1, 4), jnp.roll(vector, 1, 4),
                  jnp.roll(vector, -1, 5), jnp.roll(vector, 1, 5)]
    return 2.0 * vector + block_times(coarse_links, jnp.stack(neighbours))


def reference(source, iterate, gauge_links, clover, bc_sign, null_store, block_slot, coarse_links):
    factors = edge_factors(bc_sign, source.shape[3:])
    residual_start = source - fine_apply(iterate, gauge_links, clover, factors)
    indices = source_index(block_slot)
    coarse_rhs = restrict_all(residual_start.astype(jnp.bfloat16), null_store, indices)
    coarse_sol = RELAX_WEIGHT * coarse_rhs
    for iteration in range(CITERS - 1):
        coarse_sol = coarse_sol + RELAX_WEIGHT * (coarse_rhs - coarse_apply(coarse_sol, coarse_links))
    correction = prolong_all(coarse_sol.astype(jnp.bfloat16), null_store, indices)
    new_iterate = iterate + correction
    new_residual = residual_start - fine_apply(correction, gauge_links, clover, factors)
    return new_iterate, new_residual
```

```python
import jax
import jax.numpy as jnp
from jax import lax
from jax.experimental import pallas as pl
from jax.experimental.pallas import tpu as pltpu
from jax.sharding import PartitionSpec as P

MASS_TERM = 3.8
RELAX_WEIGHT = 0.4
NV = 24
HIGHEST = lax.Precision.HIGHEST
MESH = pl.DeviceIdType.MESH
F32 = jnp.float32

UPPER = (((0, 0), (1, 0)), ((0, 3), (1, 1)), ((1, 3), (0, 3)), ((1, 2), (0, 0)))
LOWER = (((0, 0), (1, 0)), ((0, 1), (1, 3)), ((1, 1), (0, 1)), ((1, 0), (0, 2)))


def plus_phase(a, b, power):
    power = power % 4
    if power == 0:
        return (a[0] + b[0], a[1] + b[1])
    if power == 1:
        return (a[0] - b[1], a[1] + b[0])
    if power == 2:
        return (a[0] - b[0], a[1] - b[1])
    return (a[0] + b[1], a[1] - b[0])


def spin_of(ref, spin, t):
    return (ref[0, spin, :, t], ref[1, spin, :, t])


def project(ref, t, mu, sign):
    turn = 0 if sign > 0 else 2
    return [
        plus_phase(spin_of(ref, s, t), spin_of(ref, 2 + UPPER[mu][s][0], t), UPPER[mu][s][1] + turn)
        for s in range(2)
    ]


def times_link(links, mu, t, half):
    out = [None, None]
    for b in range(3):
        ur = links[mu, 0, :, b, t]
        ui = links[mu, 1, :, b, t]
        for s in range(2):
            br = half[s][0][b][None]
            bi = half[s][1][b][None]
            re = ur * br - ui * bi
            im = ur * bi + ui * br
            out[s] = (re, im) if b == 0 else (out[s][0] + re, out[s][1] + im)
    return out


def times_dagger(links, mu, t, half):
    out = [None, None]
    for b in range(3):
        ur = links[mu, 0, b, :, t]
        ui = links[mu, 1, b, :, t]
        for s in range(2):
            br = half[s][0][b][None]
            bi = half[s][1][b][None]
            re = ur * br + ui * bi
            im = ur * bi - ui * br
            out[s] = (re, im) if b == 0 else (out[s][0] + re, out[s][1] + im)
    return out


def add_hop(total, half, mu, sign):
    turn = 0 if sign > 0 else 2
    if total is None:
        zero = jnp.zeros_like(half[0][0])
        total = [half[0], half[1], (zero, zero), (zero, zero)]
    else:
        total = [
            plus_phase(total[0], half[0], 0),
            plus_phase(total[1], half[1], 0),
            total[2],
            total[3],
        ]
    for s in range(2):
        source, power = LOWER[mu][s]
        total[2 + s] = plus_phase(total[2 + s], half[source], power + turn)
    return total


def each(half, function):
    return [(function(re), function(im)) for re, im in half]


def both(first, second, function):
    return [(function(a[0], b[0]), function(a[1], b[1])) for a, b in zip(first, second)]


def kernel(
    source_h, iterate_h, links_h, clover_h, null_h, coarse_h, bc_ref, slot_ref,
    out_x_h, out_r_h,
    source, iterate, links, clover, null_b, coarse_b, null_f, packed,
    ht, gt, gz, gx, hz_s, gz_s, hx_s, gx_s, hz_r, gz_r, hx_r, gx_r,
    part, res, corr, out_x, out_r, field, racc, rrep, coef, wbuf,
    c_t, c_z, c_x, local_sem, send_sem, recv_sem,
):
    me = (lax.axis_index("ta"), lax.axis_index("gz"), lax.axis_index("xy"))
    size = (lax.axis_size("ta"), lax.axis_size("gz"), lax.axis_size("xy"))

    def peer(axis, step):
        place = list(me)
        place[axis] = lax.rem(me[axis] + step + size[axis], size[axis])
        return tuple(place)

    loads = [
        pltpu.make_async_copy(source_from, into, local_sem.at[i])
        for i, (source_from, into) in enumerate((
            (iterate_h, iterate), (links_h, links), (clover_h, clover), (source_h, source),
            (coarse_h, coarse_b), (null_h, null_b),
        ))
    ]
    for load in loads:
        load.start()
    barrier = pltpu.get_barrier_semaphore()
    for axis in range(3):
        for step in (-1, 1):
            pl.semaphore_signal(barrier, inc=1, device_id=peer(axis, step), device_id_type=MESH)

    lane = lax.broadcasted_iota(jnp.int32, (3, 8, 128), 2)
    row = lax.broadcasted_iota(jnp.int32, (3, 8, 128), 1)
    place_y = lane % 32

    def sign_of(mu, at_edge):
        return jnp.where(at_edge, bc_ref[mu], 1).astype(F32)

    top = [sign_of(axis, me[axis] == size[axis] - 1) for axis in range(3)]
    bottom = [sign_of(axis, me[axis] == 0) for axis in range(3)]
    sign_y = bc_ref[3].astype(F32)

    def remote(phase, d, source_from, into):
        return pltpu.make_async_remote_copy(
            src_ref=source_from, dst_ref=into, send_sem=send_sem.at[phase, d],
            recv_sem=recv_sem.at[phase, d],
            device_id=peer(d // 2, -1 if d % 2 == 0 else 1), device_id_type=MESH,
        )

    def store_half(ref, index, half):
        for s in range(2):
            ref[index + (0, s)] = half[s][0]
            ref[index + (1, s)] = half[s][1]

    def load_half(ref, index):
        return [(ref[index + (0, s)], ref[index + (1, s)]) for s in range(2)]

    def fine_copies(n):
        phase = 4 * n
        return [
            remote(phase, 0, ht.at[n, 0], ht.at[n, 4]),
            remote(phase, 1, gt.at[n, 4], gt.at[n, 0]),
            remote(phase, 2, hz_s.at[n], hz_r.at[n]),
            remote(phase, 3, gz_s.at[n], gz_r.at[n]),
            remote(phase, 4, hx_s.at[n], hx_r.at[n]),
            remote(phase, 5, gx_s.at[n], gx_r.at[n]),
        ]

    def fine_send(vec, n):
        copies = fine_copies(n)

        def step_x(t, carry):
            shift_up = t * 32
            half = project(vec, t, 2, -1)
            here = lane // 32 == t
            old = load_half(hx_s, (n,))
            store_half(hx_s, (n,), both(half, old, lambda a, b: jnp.where(here, pltpu.roll(a, shift_up, 2), b)))
            back = times_dagger(links, 2, t, project(vec, t, 2, 1))
            store_half(gx, (t,), back)
            shift_down = lax.rem(t * 32 + 32, 128)
            old = load_half(gx_s, (n,))
            store_half(gx_s, (n,), both(back, old, lambda a, b: jnp.where(here, pltpu.roll(a, shift_down, 2), b)))
            return carry

        def step_t(t, carry):
            store_half(ht, (n, t), project(vec, t, 0, -1))
            store_half(gt, (n, t + 1), times_dagger(links, 0, t, project(vec, t, 0, 1)))
            return carry

        def step_z(t, carry):
            half = project(vec, t, 1, -1)
            store_half(hz_s, (n, t), each(half, lambda a: a[:, 0:1, :]))
            back = times_dagger(links, 1, t, project(vec, t, 1, 1))
            store_half(gz, (t,), back)
            store_half(gz_s, (n, t), each(back, lambda a: a[:, 7:8, :]))
            return carry

        lax.fori_loop(0, 4, step_x, 0)
        if n == 0:
            pl.semaphore_wait(barrier, 6)
        copies[4].start()
        copies[5].start()
        lax.fori_loop(0, 4, step_t, 0)
        copies[0].start()
        copies[1].start()
        lax.fori_loop(0, 4, step_z, 0)
        copies[2].start()
        copies[3].start()
        return copies

    def fine_inner(start, vec):
        def step(t, carry):
            half = project(vec, t, 3, -1)
            half = each(half, lambda a: jnp.where(place_y == 31, sign_y * pltpu.roll(a, 31, 2), pltpu.roll(a, 127, 2)))
            total = add_hop(None, times_link(links, 3, t, half), 3, -1)
            back = times_dagger(links, 3, t, project(vec, t, 3, 1))
            back = each(back, lambda a: jnp.where(place_y == 0, sign_y * pltpu.roll(a, 97, 2), pltpu.roll(a, 1, 2)))
            total = add_hop(total, back, 3, 1)
            for chirality in range(2):
                out_re = [None, None]
                out_im = [None, None]
                for column in range(6):
                    spin, colour = 2 * chirality + column // 3, column % 3
                    vr = vec[0, spin, colour, t][None]
                    vi = vec[1, spin, colour, t][None]
                    for s in range(2):
                        mr = clover[chirality, 0, 3 * s : 3 * s + 3, column, t]
                        mi = clover[chirality, 1, 3 * s : 3 * s + 3, column, t]
                        re = mr * vr - mi * vi
                        im = mr * vi + mi * vr
                        out_re[s] = re if column == 0 else out_re[s] + re
                        out_im[s] = im if column == 0 else out_im[s] + im
                for s in range(2):
                    spin = 2 * chirality + s
                    vr, vi = spin_of(vec, spin, t)
                    part[0, spin, :, t] = start[0, spin, :, t] - MASS_TERM * vr - out_re[s] + 0.5 * total[spin][0]
                    part[1, spin, :, t] = start[1, spin, :, t] - MASS_TERM * vi - out_im[s] + 0.5 * total[spin][1]
            return carry

        lax.fori_loop(0, 4, step, 0)

    def fine_outer(vec, n, out):
        def step(t, carry):
            ahead = jnp.where(t == 3, top[0], 1.0)
            behind = jnp.where(t == 0, bottom[0], 1.0)
            half = each(load_half(ht, (n, t + 1)), lambda a: a * ahead)
            total = add_hop(None, times_link(links, 0, t, half), 0, -1)
            total = add_hop(total, each(load_half(gt, (n, t)), lambda a: a * behind), 0, 1)
            edge = load_half(hz_r, (n, t))
            half = both(project(vec, t, 1, -1), edge, lambda a, b: jnp.where(row == 7, b * top[1], pltpu.roll(a, 7, 1)))
            total = add_hop(total, times_link(links, 1, t, half), 1, -1)
            edge = load_half(gz_r, (n, t))
            back = both(load_half(gz, (t,)), edge, lambda a, b: jnp.where(row == 0, b * bottom[1], pltpu.roll(a, 1, 1)))
            total = add_hop(total, back, 1, 1)
            shift = 96 - 32 * t
            edge = load_half(hx_r, (n,))
            half = both(
                project(vec, t, 2, -1), edge,
                lambda a, b: jnp.where(lane >= 96, pltpu.roll(b, shift, 2) * top[2], pltpu.roll(a, 96, 2)),
            )
            total = add_hop(total, times_link(links, 2, t, half), 2, -1)
            shift_back = lax.rem(128 - 32 * t, 128)
            edge = load_half(gx_r, (n,))
            back = both(
                load_half(gx, (t,)), edge,
                lambda a, b: jnp.where(lane < 32, pltpu.roll(b, shift_back, 2) * bottom[2], pltpu.roll(a, 32, 2)),
            )
            total = add_hop(total, back, 2, 1)
            for spin in range(4):
                out[0, spin, :, t] = part[0, spin, :, t] + 0.5 * total[spin][0]
                out[1, spin, :, t] = part[1, spin, :, t] + 0.5 * total[spin][1]
            return carry

        lax.fori_loop(0, 4, step, 0)

    loads[0].wait()
    loads[1].wait()
    first = fine_send(iterate, 0)
    loads[2].wait()
    loads[3].wait()
    fine_inner(source, iterate)

    loads[4].wait()
    gap = jnp.zeros((2, 8, 8), F32)

    def pack_step(k, carry):
        for p in range(2):
            for group in range(6):
                pieces = []
                for c in range(4):
                    pieces += [coarse_b[k, p, 4 * group + c], gap]
                packed[k, p, group] = jnp.concatenate(pieces, axis=-1)
        return carry

    lax.fori_loop(0, 9, pack_step, 0)
    loads[5].wait()

    def widen_step(v, carry):
        for k in range(2):
            for p in range(2):
                null_f[k, p, v] = null_b[k, p, v].astype(F32)
        return carry

    lax.fori_loop(0, NV, widen_step, 0)
    rrep[...] = jnp.zeros_like(rrep)
    for copy in first:
        copy.wait_recv()
    fine_outer(iterate, 0, res)

    swapped = slot_ref[0] == 1
    row2 = lax.broadcasted_iota(jnp.int32, (8, 128), 0)
    lane2 = lax.broadcasted_iota(jnp.int32, (8, 128), 1)
    spread = (lane2 % 32 // 4 == row2).astype(F32)

    def turn_step(s, carry):
        spin, colour = s // 3, lax.rem(s, 3)
        for q in range(2):
            for pair in range(2):
                first_t = res[q, spin, colour, 2 * pair].astype(jnp.bfloat16).astype(F32)
                second_t = res[q, spin, colour, 2 * pair + 1].astype(jnp.bfloat16).astype(F32)
                low = jnp.where(row2 < 4, first_t, pltpu.roll(second_t, 4, 0))
                high = jnp.where(row2 < 4, pltpu.roll(first_t, 4, 0), second_t)
                field[0, q, s, pair] = jnp.where(swapped, high, low)
                field[1, q, s, pair] = jnp.where(swapped, low, high)
        return carry

    lax.fori_loop(0, 12, turn_step, 0)

    def restrict_step(i, carry):
        k, v = i // NV, lax.rem(i, NV)
        total_re = [None, None]
        total_im = [None, None]
        for s in range(12):
            for pair in range(2):
                nr = null_f[k, 0, v, s, 8 * pair : 8 * pair + 8]
                ni = null_f[k, 1, v, s, 8 * pair : 8 * pair + 8]
                fr = field[k, 0, s, pair]
                fi = field[k, 1, s, pair]
                re = nr * fr + ni * fi
                im = nr * fi - ni * fr
                total_re[pair] = re if s == 0 else total_re[pair] + re
                total_im[pair] = im if s == 0 else total_im[pair] + im
        racc[k, 0, v] = total_re[0] + total_re[1]
        racc[k, 1, v] = total_im[0] + total_im[1]
        return carry

    lax.fori_loop(0, 2 * NV, restrict_step, 0)
    tiles = []
    for k in range(2):
        for q in range(2):
            summed = jnp.sum(racc[k, q], axis=1)
            for c in range(4):
                rrep[k, q, 32 * c : 32 * c + NV] = summed
            tiles.append(
                lax.dot_general(
                    spread, rrep[k, q], (((1,), (1,)), ((), ())), precision=HIGHEST,
                    preferred_element_type=F32,
                )
            )
    rhs = [
        [jnp.where(swapped, tiles[2 + p], tiles[p]) for p in range(2)],
        [jnp.where(swapped, tiles[p], tiles[2 + p]) for p in range(2)],
    ]

    w = [[RELAX_WEIGHT * rhs[z][p] for p in range(2)] for z in range(2)]
    lane6 = lax.broadcasted_iota(jnp.int32, (6, 8, 128), 2)
    segment = lane2 // 32
    sent = []
    for iteration in range(3):
        for z in range(2):
            for p in range(2):
                wbuf[iteration, z, p] = w[z][p]
        phase = 1 + iteration
        copies = [
            remote(phase, 0, wbuf.at[iteration], c_t.at[iteration, 0]),
            remote(phase, 1, wbuf.at[iteration], c_t.at[iteration, 1]),
            remote(phase, 2, wbuf.at[iteration, 0], c_z.at[iteration, 0]),
            remote(phase, 3, wbuf.at[iteration, 1], c_z.at[iteration, 1]),
            remote(phase, 4, wbuf.at[iteration], c_x.at[iteration, 0]),
            remote(phase, 5, wbuf.at[iteration], c_x.at[iteration, 1]),
        ]
        for copy in copies:
            copy.start()
        sent += copies
        sums = [None, None]

        def accumulate(z, k, vector):
            lr = packed[k, 0, :, z]
            li = packed[k, 1, :, z]
            wr, wi = vector[0][None], vector[1][None]
            re = lr * wr - li * wi
            im = lr * wi + li * wr
            sums[z] = (re, im) if sums[z] is None else (sums[z][0] + re, sums[z][1] + im)

        for z in range(2):
            accumulate(z, 0, w[z])
            accumulate(z, 7, [pltpu.roll(a, 7, 0) for a in w[z]])
            accumulate(z, 8, [pltpu.roll(a, 1, 0) for a in w[z]])
        accumulate(0, 3, w[1])
        accumulate(1, 4, w[0])
        for copy in copies:
            copy.wait_recv()
        for z in range(2):
            for k, ref in ((1, c_t.at[iteration, 0]), (2, c_t.at[iteration, 1]), (5, c_x.at[iteration, 0]), (6, c_x.at[iteration, 1])):
                accumulate(z, k, (ref[z, 0], ref[z, 1]))
        accumulate(1, 3, (c_z[iteration, 0, 0], c_z[iteration, 0, 1]))
        accumulate(0, 4, (c_z[iteration, 1, 0], c_z[iteration, 1, 1]))
        new = []
        for z in range(2):
            row_new = []
            for p in range(2):
                x = sums[z][p]
                for shift in (16, 8, 4, 2, 1):
                    x = x + pltpu.roll(x, 128 - shift, 2)
                row_new.append(jnp.where(lane6 % 32 == 0, x, 0.0))
            new.append(row_new)
        w = [
            [
                w[z][p] + RELAX_WEIGHT * (rhs[z][p] - (2.0 * w[z][p] + gather_lanes(new[z][p], segment)))
                for p in range(2)
            ]
            for z in range(2)
        ]

    for z in range(2):
        for p in range(2):
            chosen = jnp.where(swapped, w[1 - z][p], w[z][p]).astype(jnp.bfloat16).astype(F32)
            coef[z, p] = jnp.dot(
                jnp.transpose(chosen), spread, precision=HIGHEST, preferred_element_type=F32
            )

    def prolong_step(s, carry):
        spin, colour = s // 3, lax.rem(s, 3)
        made = []
        for k in range(2):
            total_re = [None, None]
            total_im = [None, None]
            for v in range(NV):
                cr = coef[k, 0, v : v + 1]
                ci = coef[k, 1, v : v + 1]
                for pair in range(2):
                    nr = null_f[k, 0, v, s, 8 * pair : 8 * pair + 8]
                    ni = null_f[k, 1, v, s, 8 * pair : 8 * pair + 8]
                    re = nr * cr - ni * ci
                    im = nr * ci + ni * cr
                    total_re[pair] = re if v == 0 else total_re[pair] + re
                    total_im[pair] = im if v == 0 else total_im[pair] + im
            made.append((total_re, total_im))
        for q in range(2):
            for pair in range(2):
                low = jnp.where(swapped, made[1][q][pair], made[0][q][pair])
                high = jnp.where(swapped, made[0][q][pair], made[1][q][pair])
                corr[q, spin, colour, 2 * pair] = jnp.where(row2 < 4, low, pltpu.roll(high, 4, 0))
                corr[q, spin, colour, 2 * pair + 1] = jnp.where(row2 < 4, pltpu.roll(low, 4, 0), high)
        return carry

    lax.fori_loop(0, 12, prolong_step, 0)

    second = fine_send(corr, 1)

    def add_step(t, carry):
        out_x[:, :, :, t] = iterate[:, :, :, t] + corr[:, :, :, t]
        return carry

    lax.fori_loop(0, 4, add_step, 0)
    store_x = pltpu.make_async_copy(out_x, out_x_h, local_sem.at[6])
    store_x.start()
    fine_inner(res, corr)
    for copy in second:
        copy.wait_recv()
    fine_outer(corr, 1, out_r)
    store_r = pltpu.make_async_copy(out_r, out_r_h, local_sem.at[7])
    store_r.start()
    for copy in first + sent + second:
        copy.wait_send()
    store_x.wait()
    store_r.wait()


def gather_lanes(x, segment):
    y = x[0]
    for group in range(1, 6):
        y = y + pltpu.roll(x[group], 4 * group, 1)
    placed = y
    for c in range(1, 4):
        placed = jnp.where(segment == c, pltpu.roll(y, c, 1), placed)
    placed = placed + pltpu.roll(placed, 64, 1)
    return placed + pltpu.roll(placed, 32, 1)


def per_device(source, iterate, gauge_links, clover, bc_sign, null_store, block_slot, coarse_links):
    null = null_store.reshape((2, 2, NV, 12, 16, 128))
    coarse = jnp.transpose(coarse_links, (0, 1, 2, 4, 5, 6, 7, 3)).reshape((9, 2, NV, 2, 8, NV))
    slots = block_slot.reshape((2,))
    spinor = jax.ShapeDtypeStruct((2, 4, 3, 4, 8, 128), F32)
    anywhere = pl.BlockSpec(memory_space=pl.ANY)
    scalars = pl.BlockSpec(memory_space=pltpu.SMEM)
    half = (2, 2, 3, 8, 128)
    vmem = lambda *shape: pltpu.VMEM(shape, F32)
    return pl.pallas_call(
        kernel,
        out_shape=(spinor, spinor),
        in_specs=[anywhere] * 6 + [scalars] * 2,
        out_specs=(anywhere, anywhere),
        scratch_shapes=[
            vmem(*spinor.shape), vmem(*spinor.shape), vmem(4, 2, 3, 3, 4, 8, 128),
            vmem(2, 2, 6, 6, 4, 8, 128), pltpu.VMEM((2, 2, NV, 12, 16, 128), jnp.bfloat16),
            vmem(9, 2, NV, 2, 8, NV), vmem(2, 2, NV, 12, 16, 128), vmem(9, 2, 6, 2, 8, 128),
            vmem(2, 5, *half), vmem(2, 5, *half), vmem(4, *half), vmem(4, *half),
            vmem(2, 4, 2, 2, 3, 1, 128), vmem(2, 4, 2, 2, 3, 1, 128), vmem(2, *half), vmem(2, *half),
            vmem(2, 4, 2, 2, 3, 1, 128), vmem(2, 4, 2, 2, 3, 1, 128), vmem(2, *half), vmem(2, *half),
            vmem(*spinor.shape), vmem(*spinor.shape), vmem(*spinor.shape), vmem(*spinor.shape),
            vmem(*spinor.shape), vmem(2, 2, 12, 2, 8, 128), vmem(2, 2, NV, 8, 128),
            vmem(2, 2, 128, 128), vmem(2, 2, 128, 128), vmem(3, 2, 2, 8, 128),
            vmem(3, 2, 2, 2, 8, 128), vmem(3, 2, 2, 8, 128), vmem(3, 2, 2, 2, 8, 128),
            pltpu.SemaphoreType.DMA((8,)), pltpu.SemaphoreType.DMA((5, 6)),
            pltpu.SemaphoreType.DMA((5, 6)),
        ],
        compiler_params=pltpu.CompilerParams(
            collective_id=0, has_side_effects=True, vmem_limit_bytes=60 * 1024 * 1024
        ),
    )(source, iterate, gauge_links, clover, null, coarse, bc_sign, slots)


def solution(mesh):
    spinor = P(None, None, None, "ta", "gz", "xy")
    matrix = P(None, None, None, None, "ta", "gz", "xy")
    column = P("ta", "gz", "xy", None, None, None, None, None, None)
    placed = (
        spinor, spinor, matrix, matrix, P(), column, P("ta", "gz", "xy"),
        P(None, None, None, None, "ta", "gz", "xy", None),
    )
    return jax.shard_map(
        per_device, mesh=mesh, in_specs=placed, out_specs=(spinor, spinor), check_vma=False
    )
```

```python
import jax
import jax.numpy as jnp
from jax import lax
from jax.experimental import pallas as pl
from jax.experimental.pallas import tpu as pltpu
from jax.sharding import PartitionSpec as P

MASS_TERM = 3.8
RELAX_WEIGHT = 0.4
NV = 24
HIGHEST = lax.Precision.HIGHEST
MESH = pl.DeviceIdType.MESH
F32 = jnp.float32

UPPER = (((0, 0), (1, 0)), ((0, 3), (1, 1)), ((1, 3), (0, 3)), ((1, 2), (0, 0)))
LOWER = (((0, 0), (1, 0)), ((0, 1), (1, 3)), ((1, 1), (0, 1)), ((1, 0), (0, 2)))


def plus_phase(a, b, power):
    power = power % 4
    if power == 0:
        return (a[0] + b[0], a[1] + b[1])
    if power == 1:
        return (a[0] - b[1], a[1] + b[0])
    if power == 2:
        return (a[0] - b[0], a[1] - b[1])
    return (a[0] + b[1], a[1] - b[0])


def spin_of(ref, spin, t):
    return (ref[0, spin, :, t], ref[1, spin, :, t])


def project(ref, t, mu, sign):
    turn = 0 if sign > 0 else 2
    return [
        plus_phase(spin_of(ref, s, t), spin_of(ref, 2 + UPPER[mu][s][0], t), UPPER[mu][s][1] + turn)
        for s in range(2)
    ]


def times_link(links, mu, t, half):
    out = [None, None]
    for b in range(3):
        ur = links[mu, 0, :, b, t]
        ui = links[mu, 1, :, b, t]
        for s in range(2):
            br = half[s][0][b][None]
            bi = half[s][1][b][None]
            re = ur * br - ui * bi
            im = ur * bi + ui * br
            out[s] = (re, im) if b == 0 else (out[s][0] + re, out[s][1] + im)
    return out


def times_dagger(links, mu, t, half):
    out = [None, None]
    for b in range(3):
        ur = links[mu, 0, b, :, t]
        ui = links[mu, 1, b, :, t]
        for s in range(2):
            br = half[s][0][b][None]
            bi = half[s][1][b][None]
            re = ur * br + ui * bi
            im = ur * bi - ui * br
            out[s] = (re, im) if b == 0 else (out[s][0] + re, out[s][1] + im)
    return out


def add_hop(total, half, mu, sign):
    turn = 0 if sign > 0 else 2
    if total is None:
        zero = jnp.zeros_like(half[0][0])
        total = [half[0], half[1], (zero, zero), (zero, zero)]
    else:
        total = [
            plus_phase(total[0], half[0], 0),
            plus_phase(total[1], half[1], 0),
            total[2],
            total[3],
        ]
    for s in range(2):
        source, power = LOWER[mu][s]
        total[2 + s] = plus_phase(total[2 + s], half[source], power + turn)
    return total


def each(half, function):
    return [(function(re), function(im)) for re, im in half]


def both(first, second, function):
    return [(function(a[0], b[0]), function(a[1], b[1])) for a, b in zip(first, second)]


def kernel(
    source_h, iterate_h, links_h, clover_h, null_h, coarse_h, bc_ref, slot_ref,
    out_x, out_r,
    source, iterate, links, clover, null_b, coarse_b, packed,
    ht, gt, gz, gx, hz_s, gz_s, hx_s, gx_s, hz_r, gz_r, hx_r, gx_r,
    part, res, corr, wide, field, rrow, coef, tile, wbuf,
    c_halo, local_sem, send_sem, recv_sem,
):
    me = (lax.axis_index("ta"), lax.axis_index("gz"), lax.axis_index("xy"))
    size = (lax.axis_size("ta"), lax.axis_size("gz"), lax.axis_size("xy"))

    def peer(axis, step):
        place = list(me)
        place[axis] = lax.rem(me[axis] + step + size[axis], size[axis])
        return tuple(place)

    loads = [
        pltpu.make_async_copy(source_from, into, local_sem.at[i])
        for i, (source_from, into) in enumerate((
            (iterate_h, iterate), (links_h, links), (clover_h, clover), (source_h, source),
            (coarse_h, coarse_b), (null_h, null_b),
        ))
    ]
    for load in loads:
        load.start()
    barrier = pltpu.get_barrier_semaphore()
    for axis in range(3):
        for step in (-1, 1):
            pl.semaphore_signal(barrier, inc=1, device_id=peer(axis, step), device_id_type=MESH)

    lane = lax.broadcasted_iota(jnp.int32, (3, 8, 128), 2)
    row = lax.broadcasted_iota(jnp.int32, (3, 8, 128), 1)
    place_y = lane % 32

    def sign_of(mu, at_edge):
        return jnp.where(at_edge, bc_ref[mu], 1).astype(F32)

    top = [sign_of(axis, me[axis] == size[axis] - 1) for axis in range(3)]
    bottom = [sign_of(axis, me[axis] == 0) for axis in range(3)]
    sign_y = bc_ref[3].astype(F32)

    def remote(phase, d, source_from, into):
        return pltpu.make_async_remote_copy(
            src_ref=source_from, dst_ref=into, send_sem=send_sem.at[phase, d],
            recv_sem=recv_sem.at[phase, d],
            device_id=peer(d // 2, -1 if d % 2 == 0 else 1), device_id_type=MESH,
        )

    def store_half(ref, index, half):
        for s in range(2):
            ref[index + (0, s)] = half[s][0]
            ref[index + (1, s)] = half[s][1]

    def load_half(ref, index):
        return [(ref[index + (0, s)], ref[index + (1, s)]) for s in range(2)]

    def fine_copies(n):
        phase = 4 * n
        return [
            remote(phase, 0, ht.at[n, 0], ht.at[n, 4]),
            remote(phase, 1, gt.at[n, 4], gt.at[n, 0]),
            remote(phase, 2, hz_s.at[n], hz_r.at[n]),
            remote(phase, 3, gz_s.at[n], gz_r.at[n]),
            remote(phase, 4, hx_s.at[n], hx_r.at[n]),
            remote(phase, 5, gx_s.at[n], gx_r.at[n]),
        ]

    def fine_send(vec, n):
        copies = fine_copies(n)

        def step_x(t, carry):
            shift_up = t * 32
            half = project(vec, t, 2, -1)
            here = lane // 32 == t
            old = load_half(hx_s, (n,))
            store_half(hx_s, (n,), both(half, old, lambda a, b: jnp.where(here, pltpu.roll(a, shift_up, 2), b)))
            back = times_dagger(links, 2, t, project(vec, t, 2, 1))
            store_half(gx, (t,), back)
            shift_down = lax.rem(t * 32 + 32, 128)
            old = load_half(gx_s, (n,))
            store_half(gx_s, (n,), both(back, old, lambda a, b: jnp.where(here, pltpu.roll(a, shift_down, 2), b)))
            return carry

        def step_t(t, carry):
            store_half(ht, (n, t + 1), project(vec, t + 1, 0, -1))
            store_half(gt, (n, t + 1), times_dagger(links, 0, t, project(vec, t, 0, 1)))
            return carry

        def step_z(t, carry):
            half = project(vec, t, 1, -1)
            store_half(hz_s, (n, t), each(half, lambda a: a[:, 0:1, :]))
            back = times_dagger(links, 1, t, project(vec, t, 1, 1))
            store_half(gz, (t,), back)
            store_half(gz_s, (n, t), each(back, lambda a: a[:, 7:8, :]))
            return carry

        store_half(ht, (n, 0), project(vec, 0, 0, -1))
        store_half(gt, (n, 4), times_dagger(links, 0, 3, project(vec, 3, 0, 1)))
        if n == 0:
            pl.semaphore_wait(barrier, 6)
        copies[0].start()
        copies[1].start()
        lax.fori_loop(0, 4, step_x, 0)
        copies[4].start()
        copies[5].start()
        lax.fori_loop(0, 4, step_z, 0)
        copies[2].start()
        copies[3].start()
        lax.fori_loop(0, 3, step_t, 0)
        return copies

    def fine_inner(start, vec):
        def step(t, carry):
            half = project(vec, t, 3, -1)
            half = each(half, lambda a: jnp.where(place_y == 31, sign_y * pltpu.roll(a, 31, 2), pltpu.roll(a, 127, 2)))
            total = add_hop(None, times_link(links, 3, t, half), 3, -1)
            back = times_dagger(links, 3, t, project(vec, t, 3, 1))
            back = each(back, lambda a: jnp.where(place_y == 0, sign_y * pltpu.roll(a, 97, 2), pltpu.roll(a, 1, 2)))
            total = add_hop(total, back, 3, 1)
            for chirality in range(2):
                out_re = [None, None]
                out_im = [None, None]
                for column in range(6):
                    spin, colour = 2 * chirality + column // 3, column % 3
                    vr = vec[0, spin, colour, t][None]
                    vi = vec[1, spin, colour, t][None]
                    for s in range(2):
                        mr = clover[chirality, 0, 3 * s : 3 * s + 3, column, t]
                        mi = clover[chirality, 1, 3 * s : 3 * s + 3, column, t]
                        re = mr * vr - mi * vi
                        im = mr * vi + mi * vr
                        out_re[s] = re if column == 0 else out_re[s] + re
                        out_im[s] = im if column == 0 else out_im[s] + im
                for s in range(2):
                    spin = 2 * chirality + s
                    vr, vi = spin_of(vec, spin, t)
                    part[0, spin, :, t] = start[0, spin, :, t] - MASS_TERM * vr - out_re[s] + 0.5 * total[spin][0]
                    part[1, spin, :, t] = start[1, spin, :, t] - MASS_TERM * vi - out_im[s] + 0.5 * total[spin][1]
            return carry

        lax.fori_loop(0, 4, step, 0)

    def fine_outer(vec, n, out, keep):
        def step(t, carry):
            ahead = jnp.where(t == 3, top[0], 1.0)
            behind = jnp.where(t == 0, bottom[0], 1.0)
            half = each(load_half(ht, (n, t + 1)), lambda a: a * ahead)
            total = add_hop(None, times_link(links, 0, t, half), 0, -1)
            total = add_hop(total, each(load_half(gt, (n, t)), lambda a: a * behind), 0, 1)
            edge = load_half(hz_r, (n, t))
            half = both(project(vec, t, 1, -1), edge, lambda a, b: jnp.where(row == 7, b * top[1], pltpu.roll(a, 7, 1)))
            total = add_hop(total, times_link(links, 1, t, half), 1, -1)
            edge = load_half(gz_r, (n, t))
            back = both(load_half(gz, (t,)), edge, lambda a, b: jnp.where(row == 0, b * bottom[1], pltpu.roll(a, 1, 1)))
            total = add_hop(total, back, 1, 1)
            shift = 96 - 32 * t
            edge = load_half(hx_r, (n,))
            half = both(
                project(vec, t, 2, -1), edge,
                lambda a, b: jnp.where(lane >= 96, pltpu.roll(b, shift, 2) * top[2], pltpu.roll(a, 96, 2)),
            )
            total = add_hop(total, times_link(links, 2, t, half), 2, -1)
            shift_back = lax.rem(128 - 32 * t, 128)
            edge = load_half(gx_r, (n,))
            back = both(
                load_half(gx, (t,)), edge,
                lambda a, b: jnp.where(lane < 32, pltpu.roll(b, shift_back, 2) * bottom[2], pltpu.roll(a, 32, 2)),
            )
            total = add_hop(total, back, 2, 1)
            for spin in range(4):
                for q in range(2):
                    value = part[q, spin, :, t] + 0.5 * total[spin][q]
                    out[q, spin, :, t] = value
                    if keep:
                        start = pl.multiple_of(4 * t, 4)
                        for z in range(2):
                            for colour in range(3):
                                wide[z, q, 3 * spin + colour, pl.ds(start, 4)] = value[colour, 4 * z : 4 * z + 4]
            return carry

        lax.fori_loop(0, 4, step, 0)

    loads[0].wait()
    loads[1].wait()
    first = fine_send(iterate, 0)
    loads[2].wait()
    loads[3].wait()
    fine_inner(source, iterate)

    loads[4].wait()
    gap = jnp.zeros((8, 8), F32)

    def pack_step(k, carry):
        for i in range(NV):
            pieces = []
            for p in range(2):
                for z in range(2):
                    pieces += [coarse_b[k, p, i, z], gap]
            packed[k, i] = jnp.concatenate(pieces, axis=-1)
        return carry

    lax.fori_loop(0, 9, pack_step, 0)
    loads[5].wait()
    rrow[...] = jnp.zeros_like(rrow)
    for copy in first:
        copy.wait_recv()
    fine_outer(iterate, 0, res, True)

    row2 = lax.broadcasted_iota(jnp.int32, (8, 128), 0)
    lane2 = lax.broadcasted_iota(jnp.int32, (8, 128), 1)
    spread = (lane2 % 32 // 4 == row2).astype(F32)

    def round_step(s, carry):
        for z in range(2):
            re = wide[z, 0, s].astype(jnp.bfloat16)
            im = wide[z, 1, s].astype(jnp.bfloat16)
            field[z, 0, s] = re
            field[z, 1, s] = im
            field[z, 2, s] = -re
        return carry

    lax.fori_loop(0, 12, round_step, 0)

    def running(total, a, b):
        product = a.astype(F32) * b.astype(F32)
        return product if total is None else total + product

    for z in range(2):
        slot = slot_ref[z]

        def restrict_step(i, carry):
            totals = [[None, None], [None, None]]
            for s in range(12):
                for u in range(2):
                    nr = null_b[slot, 0, 2 * i + u, s]
                    ni = null_b[slot, 1, 2 * i + u, s]
                    totals[u][0] = running(totals[u][0], nr, field[z, 0, s])
                    totals[u][1] = running(totals[u][1], nr, field[z, 1, s])
                    totals[u][0] = running(totals[u][0], ni, field[z, 1, s])
                    totals[u][1] = running(totals[u][1], ni, field[z, 2, s])
            for u in range(2):
                for q in range(2):
                    rrow[pl.ds(64 * q + 32 * z + 2 * i + u, 1)] = jnp.sum(totals[u][q], axis=0, keepdims=True)
            return carry

        lax.fori_loop(0, NV // 2, restrict_step, 0)

    rhs = lax.dot_general(
        spread, rrow[...], (((1,), (1,)), ((), ())), precision=HIGHEST, preferred_element_type=F32
    )
    w = RELAX_WEIGHT * rhs
    lower_z = lane2 % 64 < 32
    lower_p = lane2 < 64
    parity = jnp.where(lower_p, 1.0, -1.0)

    def accumulate(sums, k, vector):
        blocks = packed[k]
        re = blocks * (vector * parity)[None]
        im = blocks * pltpu.roll(vector, 64, 1)[None]
        return (re, im) if sums is None else (sums[0] + re, sums[1] + im)

    def folded(low, high, distance):
        lanes = lax.broadcasted_iota(jnp.int32, low.shape, low.ndim - 1)
        clear = lanes // distance % 2 == 0
        axis = low.ndim - 1
        return jnp.where(clear, low, pltpu.roll(high, distance, axis)) + jnp.where(
            clear, pltpu.roll(low, 128 - distance, axis), high
        )

    sent = []
    for iteration in range(3):
        wbuf[iteration] = w
        phase = 1 + iteration
        copies = [
            remote(phase, d, wbuf.at[iteration], c_halo.at[iteration, d]) for d in range(6)
        ]
        for copy in copies:
            copy.start()
        sent += copies
        sums = accumulate(None, 0, w)
        sums = accumulate(sums, 7, pltpu.roll(w, 7, 0))
        sums = accumulate(sums, 8, pltpu.roll(w, 1, 0))
        for copy in copies:
            copy.wait_recv()
        sums = accumulate(sums, 1, c_halo[iteration, 0])
        sums = accumulate(sums, 2, c_halo[iteration, 1])
        sums = accumulate(sums, 5, c_halo[iteration, 4])
        sums = accumulate(sums, 6, c_halo[iteration, 5])
        ahead = jnp.where(lower_z, pltpu.roll(w, 96, 1), pltpu.roll(c_halo[iteration, 2], 32, 1))
        sums = accumulate(sums, 3, ahead)
        behind = jnp.where(lower_z, pltpu.roll(c_halo[iteration, 3], 96, 1), pltpu.roll(w, 32, 1))
        sums = accumulate(sums, 4, behind)
        wide_p = lax.broadcasted_iota(jnp.int32, (NV, 8, 128), 2) < 64
        folds = jnp.where(wide_p, sums[0], sums[1]) + pltpu.roll(jnp.where(wide_p, sums[1], sums[0]), 64, 2)
        middle = folds[8:16]
        bit = lax.broadcasted_iota(jnp.int32, (8, 8, 128), 2) // 16 % 2 == 0
        middle = jnp.where(bit, middle + pltpu.roll(middle, 112, 2), 0.0)
        folds = folded(folded(folds[0:8], folds[16:24], 16), middle, 8)
        folds = folded(folds[0:4], folds[4:8], 4)
        folds = folded(folds[0:2], folds[2:4], 2)
        total = folded(folds[0], folds[1], 1)
        w = w + RELAX_WEIGHT * (rhs - (2.0 * w + total))

    coef[...] = jnp.dot(
        jnp.transpose(w.astype(jnp.bfloat16).astype(F32)), spread, preferred_element_type=F32
    )
    def tile_step(v, carry):
        for z in range(2):
            re = jnp.broadcast_to(coef[pl.ds(32 * z + v, 1)], (16, 128))
            im = jnp.broadcast_to(coef[pl.ds(64 + 32 * z + v, 1)], (16, 128))
            for kind, value in enumerate((re, im, -im)):
                tile[z, kind, v] = value.astype(jnp.bfloat16)
        return carry

    lax.fori_loop(0, NV, tile_step, 0)

    for z in range(2):
        slot = slot_ref[z]

        def prolong_step(i, carry):
            totals = [[None, None], [None, None]]
            for v in range(NV):
                for p in range(2):
                    for u in range(2):
                        null = null_b[slot, p, v, 2 * i + u]
                        for q in range(2):
                            kind = ((0, 2), (1, 0))[q][p]
                            totals[u][q] = running(totals[u][q], null, tile[z, kind, v])
            for u in range(2):
                s = 2 * i + u
                spin, colour = s // 3, lax.rem(s, 3)
                for q in range(2):
                    for t in range(4):
                        corr[q, spin, colour, t, 4 * z : 4 * z + 4] = totals[u][q][4 * t : 4 * t + 4]
            return carry

        lax.fori_loop(0, 6, prolong_step, 0)

    second = fine_send(corr, 1)

    def add_step(t, carry):
        out_x[:, :, :, t] = iterate[:, :, :, t] + corr[:, :, :, t]
        return carry

    lax.fori_loop(0, 4, add_step, 0)
    fine_inner(res, corr)
    for copy in second:
        copy.wait_recv()
    fine_outer(corr, 1, out_r, False)
    for copy in first + sent + second:
        copy.wait_send()


def per_device(source, iterate, gauge_links, clover, bc_sign, null_store, block_slot, coarse_links):
    null = null_store.reshape((2, 2, NV, 12, 16, 128))
    coarse = jnp.transpose(coarse_links, (0, 1, 2, 4, 5, 6, 7, 3)).reshape((9, 2, NV, 2, 8, NV))
    slots = block_slot.reshape((2,))
    spinor = pltpu.VMEM((2, 4, 3, 4, 8, 128), F32)
    anywhere = pl.BlockSpec(memory_space=pl.ANY)
    scalars = pl.BlockSpec(memory_space=pltpu.SMEM)
    half = (2, 2, 3, 8, 128)
    vmem = lambda *shape: pltpu.VMEM(shape, F32)
    return pl.pallas_call(
        kernel,
        out_shape=(spinor, spinor),
        in_specs=[anywhere] * 6 + [scalars] * 2,
        out_specs=(pl.BlockSpec(memory_space=pltpu.VMEM),) * 2,
        scratch_shapes=[
            vmem(*spinor.shape), vmem(*spinor.shape), vmem(4, 2, 3, 3, 4, 8, 128),
            vmem(2, 2, 6, 6, 4, 8, 128), pltpu.VMEM((2, 2, NV, 12, 16, 128), jnp.bfloat16),
            vmem(9, 2, NV, 2, 8, NV), vmem(9, NV, 8, 128),
            vmem(2, 5, *half), vmem(2, 5, *half), vmem(4, *half), vmem(4, *half),
            vmem(2, 4, 2, 2, 3, 1, 128), vmem(2, 4, 2, 2, 3, 1, 128), vmem(2, *half), vmem(2, *half),
            vmem(2, 4, 2, 2, 3, 1, 128), vmem(2, 4, 2, 2, 3, 1, 128), vmem(2, *half), vmem(2, *half),
            vmem(*spinor.shape), vmem(*spinor.shape), vmem(*spinor.shape), vmem(2, 2, 12, 16, 128),
            pltpu.VMEM((2, 3, 12, 16, 128), jnp.bfloat16), vmem(128, 128), vmem(128, 128),
            pltpu.VMEM((2, 3, NV, 16, 128), jnp.bfloat16), vmem(3, 8, 128), vmem(3, 6, 8, 128),
            pltpu.SemaphoreType.DMA((6,)), pltpu.SemaphoreType.DMA((5, 6)),
            pltpu.SemaphoreType.DMA((5, 6)),
        ],
        compiler_params=pltpu.CompilerParams(
            collective_id=0, has_side_effects=True, vmem_limit_bytes=56 * 1024 * 1024
        ),
    )(source, iterate, gauge_links, clover, null, coarse, bc_sign, slots)


def solution(mesh):
    spinor = P(None, None, None, "ta", "gz", "xy")
    matrix = P(None, None, None, None, "ta", "gz", "xy")
    column = P("ta", "gz", "xy", None, None, None, None, None, None)
    placed = (
        spinor, spinor, matrix, matrix, P(), column, P("ta", "gz", "xy"),
        P(None, None, None, None, "ta", "gz", "xy", None),
    )
    return jax.shard_map(
        per_device, mesh=mesh, in_specs=placed, out_specs=(spinor, spinor), check_vma=False
    )
```

```python
import jax
import jax.numpy as jnp
from jax import lax
from jax.experimental import pallas as pl
from jax.experimental.pallas import tpu as pltpu
from jax.sharding import PartitionSpec as P

MASS_TERM = 3.8
RELAX_WEIGHT = 0.4
NV = 24
HIGHEST = lax.Precision.HIGHEST
MESH = pl.DeviceIdType.MESH
F32 = jnp.float32

UPPER = (((0, 0), (1, 0)), ((0, 3), (1, 1)), ((1, 3), (0, 3)), ((1, 2), (0, 0)))
LOWER = (((0, 0), (1, 0)), ((0, 1), (1, 3)), ((1, 1), (0, 1)), ((1, 0), (0, 2)))


def plus_phase(a, b, power):
    power = power % 4
    if power == 0:
        return (a[0] + b[0], a[1] + b[1])
    if power == 1:
        return (a[0] - b[1], a[1] + b[0])
    if power == 2:
        return (a[0] - b[0], a[1] - b[1])
    return (a[0] + b[1], a[1] - b[0])


def spin_of(ref, spin, t):
    return (ref[0, spin, :, t], ref[1, spin, :, t])


def project(ref, t, mu, sign):
    turn = 0 if sign > 0 else 2
    return [
        plus_phase(spin_of(ref, s, t), spin_of(ref, 2 + UPPER[mu][s][0], t), UPPER[mu][s][1] + turn)
        for s in range(2)
    ]


def times_link(links, mu, t, half):
    out = [None, None]
    for b in range(3):
        ur = links[mu, 0, :, b, t]
        ui = links[mu, 1, :, b, t]
        for s in range(2):
            br = half[s][0][b][None]
            bi = half[s][1][b][None]
            re = ur * br - ui * bi
            im = ur * bi + ui * br
            out[s] = (re, im) if b == 0 else (out[s][0] + re, out[s][1] + im)
    return out


def times_dagger(links, mu, t, half):
    out = [None, None]
    for b in range(3):
        ur = links[mu, 0, b, :, t]
        ui = links[mu, 1, b, :, t]
        for s in range(2):
            br = half[s][0][b][None]
            bi = half[s][1][b][None]
            re = ur * br + ui * bi
            im = ur * bi - ui * br
            out[s] = (re, im) if b == 0 else (out[s][0] + re, out[s][1] + im)
    return out


def add_hop(total, half, mu, sign):
    turn = 0 if sign > 0 else 2
    if total is None:
        zero = jnp.zeros_like(half[0][0])
        total = [half[0], half[1], (zero, zero), (zero, zero)]
    else:
        total = [
            plus_phase(total[0], half[0], 0),
            plus_phase(total[1], half[1], 0),
            total[2],
            total[3],
        ]
    for s in range(2):
        source, power = LOWER[mu][s]
        total[2 + s] = plus_phase(total[2 + s], half[source], power + turn)
    return total


def each(half, function):
    return [(function(re), function(im)) for re, im in half]


def both(first, second, function):
    return [(function(a[0], b[0]), function(a[1], b[1])) for a, b in zip(first, second)]


def kernel(
    source_h, iterate_h, links_h, clover_h, null_h, coarse_h, bc_h, slot_h,
    out_x, out_r,
    source, iterate, links, clover, null_b, coarse_b, packed,
    ht, gt, gz, gx, hz_s, gz_s, hx_s, gx_s, hz_r, gz_r, hx_r, gx_r,
    part, res, corr, wide, field, rrow, coef, tile, wbuf,
    c_halo, bc_ref, slot_ref, local_sem, send_sem, recv_sem,
):
    me = (lax.axis_index("ta"), lax.axis_index("gz"), lax.axis_index("xy"))
    size = (lax.axis_size("ta"), lax.axis_size("gz"), lax.axis_size("xy"))

    def peer(axis, step):
        place = list(me)
        place[axis] = lax.rem(me[axis] + step + size[axis], size[axis])
        return tuple(place)

    loads = [
        pltpu.make_async_copy(source_from, into, local_sem.at[i])
        for i, (source_from, into) in enumerate((
            (iterate_h, iterate), (links_h.at[0:3], links.at[0:3]), (clover_h, clover), (source_h, source),
            (coarse_h, coarse_b), (null_h, null_b), (links_h.at[3], links.at[3]),
            (bc_h, bc_ref), (slot_h, slot_ref),
        ))
    ]
    loads[0].start()
    loads[1].start()
    barrier = pltpu.get_barrier_semaphore()
    for axis in range(3):
        for step in (-1, 1):
            pl.semaphore_signal(barrier, inc=1, device_id=peer(axis, step), device_id_type=MESH)

    lane = lax.broadcasted_iota(jnp.int32, (3, 8, 128), 2)
    row = lax.broadcasted_iota(jnp.int32, (3, 8, 128), 1)
    place_y = lane % 32

    def sign_of(mu, at_edge):
        return jnp.where(at_edge, bc_ref[mu], 1).astype(F32)

    def remote(phase, d, source_from, into):
        return pltpu.make_async_remote_copy(
            src_ref=source_from, dst_ref=into, send_sem=send_sem.at[phase, d],
            recv_sem=recv_sem.at[phase, d],
            device_id=peer(d // 2, -1 if d % 2 == 0 else 1), device_id_type=MESH,
        )

    def store_half(ref, index, half):
        for s in range(2):
            ref[index + (0, s)] = half[s][0]
            ref[index + (1, s)] = half[s][1]

    def load_half(ref, index):
        return [(ref[index + (0, s)], ref[index + (1, s)]) for s in range(2)]

    def fine_copies(n):
        phase = 4 * n
        return [
            remote(phase, 0, ht.at[n, 0], ht.at[n, 4]),
            remote(phase, 1, gt.at[n, 4], gt.at[n, 0]),
            remote(phase, 2, hz_s.at[n], hz_r.at[n]),
            remote(phase, 3, gz_s.at[n], gz_r.at[n]),
            remote(phase, 4, hx_s.at[n], hx_r.at[n]),
            remote(phase, 5, gx_s.at[n], gx_r.at[n]),
        ]

    def fine_send(vec, n):
        copies = fine_copies(n)

        def send_x():
            ahead = None
            behind = None
            for t in range(4):
                here = lane // 32 == t
                half = project(vec, t, 2, -1)
                back = times_dagger(links, 2, t, project(vec, t, 2, 1))
                store_half(gx, (t,), back)
                half = each(half, lambda a: pltpu.roll(a, 32 * t, 2) if t else a)
                back = each(back, lambda a: pltpu.roll(a, (32 * t + 32) % 128, 2) if t < 3 else a)
                ahead = half if t == 0 else both(half, ahead, lambda a, b: jnp.where(here, a, b))
                behind = back if t == 0 else both(back, behind, lambda a, b: jnp.where(here, a, b))
            store_half(hx_s, (n,), ahead)
            store_half(gx_s, (n,), behind)

        def step_t(t, carry):
            store_half(ht, (n, t + 1), project(vec, t + 1, 0, -1))
            store_half(gt, (n, t + 1), times_dagger(links, 0, t, project(vec, t, 0, 1)))
            return carry

        def step_z(t, carry):
            half = project(vec, t, 1, -1)
            store_half(hz_s, (n, t), each(half, lambda a: a[:, 0:1, :]))
            back = times_dagger(links, 1, t, project(vec, t, 1, 1))
            store_half(gz, (t,), back)
            store_half(gz_s, (n, t), each(back, lambda a: a[:, 7:8, :]))
            return carry

        store_half(ht, (n, 0), project(vec, 0, 0, -1))
        store_half(gt, (n, 4), times_dagger(links, 0, 3, project(vec, 3, 0, 1)))
        if n == 0:
            pl.semaphore_wait(barrier, 6)
        copies[0].start()
        copies[1].start()
        send_x()
        copies[4].start()
        copies[5].start()
        for t in range(4):
            step_z(t, 0)
        copies[2].start()
        copies[3].start()
        lax.fori_loop(0, 3, step_t, 0)
        return copies

    def fine_inner(start, vec):
        def step(t, carry):
            half = project(vec, t, 3, -1)
            half = each(half, lambda a: jnp.where(place_y == 31, sign_y * pltpu.roll(a, 31, 2), pltpu.roll(a, 127, 2)))
            total = add_hop(None, times_link(links, 3, t, half), 3, -1)
            back = times_dagger(links, 3, t, project(vec, t, 3, 1))
            back = each(back, lambda a: jnp.where(place_y == 0, sign_y * pltpu.roll(a, 97, 2), pltpu.roll(a, 1, 2)))
            total = add_hop(total, back, 3, 1)
            for chirality in range(2):
                out_re = [None, None]
                out_im = [None, None]
                for column in range(6):
                    spin, colour = 2 * chirality + column // 3, column % 3
                    vr = vec[0, spin, colour, t][None]
                    vi = vec[1, spin, colour, t][None]
                    for s in range(2):
                        mr = clover[chirality, 0, 3 * s : 3 * s + 3, column, t]
                        mi = clover[chirality, 1, 3 * s : 3 * s + 3, column, t]
                        re = mr * vr - mi * vi
                        im = mr * vi + mi * vr
                        out_re[s] = re if column == 0 else out_re[s] + re
                        out_im[s] = im if column == 0 else out_im[s] + im
                for s in range(2):
                    spin = 2 * chirality + s
                    vr, vi = spin_of(vec, spin, t)
                    part[0, spin, :, t] = start[0, spin, :, t] - MASS_TERM * vr - out_re[s] + 0.5 * total[spin][0]
                    part[1, spin, :, t] = start[1, spin, :, t] - MASS_TERM * vi - out_im[s] + 0.5 * total[spin][1]
            return carry

        lax.fori_loop(0, 4, step, 0)

    def fine_outer(vec, n, out, keep):
        def step(t, carry):
            ahead = jnp.where(t == 3, top[0], 1.0)
            behind = jnp.where(t == 0, bottom[0], 1.0)
            half = each(load_half(ht, (n, t + 1)), lambda a: a * ahead)
            total = add_hop(None, times_link(links, 0, t, half), 0, -1)
            total = add_hop(total, each(load_half(gt, (n, t)), lambda a: a * behind), 0, 1)
            edge = load_half(hz_r, (n, t))
            half = both(project(vec, t, 1, -1), edge, lambda a, b: jnp.where(row == 7, b * top[1], pltpu.roll(a, 7, 1)))
            total = add_hop(total, times_link(links, 1, t, half), 1, -1)
            edge = load_half(gz_r, (n, t))
            back = both(load_half(gz, (t,)), edge, lambda a, b: jnp.where(row == 0, b * bottom[1], pltpu.roll(a, 1, 1)))
            total = add_hop(total, back, 1, 1)
            shift = 96 - 32 * t
            edge = load_half(hx_r, (n,))
            half = both(
                project(vec, t, 2, -1), edge,
                lambda a, b: jnp.where(lane >= 96, pltpu.roll(b, shift, 2) * top[2], pltpu.roll(a, 96, 2)),
            )
            total = add_hop(total, times_link(links, 2, t, half), 2, -1)
            shift_back = lax.rem(128 - 32 * t, 128)
            edge = load_half(gx_r, (n,))
            back = both(
                load_half(gx, (t,)), edge,
                lambda a, b: jnp.where(lane < 32, pltpu.roll(b, shift_back, 2) * bottom[2], pltpu.roll(a, 32, 2)),
            )
            total = add_hop(total, back, 2, 1)
            for spin in range(4):
                for q in range(2):
                    value = part[q, spin, :, t] + 0.5 * total[spin][q]
                    out[q, spin, :, t] = value
                    if keep:
                        start = pl.multiple_of(4 * t, 4)
                        for z in range(2):
                            for colour in range(3):
                                wide[z, q, 3 * spin + colour, pl.ds(start, 4)] = value[colour, 4 * z : 4 * z + 4]
            return carry

        lax.fori_loop(0, 4, step, 0)

    loads[0].wait()
    loads[1].wait()
    for i in (7, 8, 6, 2, 3, 4, 5):
        loads[i].start()
    first = fine_send(iterate, 0)
    for i in (7, 8, 6, 2):
        loads[i].wait()
    loads[3].wait()
    top = [sign_of(axis, me[axis] == size[axis] - 1) for axis in range(3)]
    bottom = [sign_of(axis, me[axis] == 0) for axis in range(3)]
    sign_y = bc_ref[3].astype(F32)
    fine_inner(source, iterate)

    loads[4].wait()
    gap = jnp.zeros((8, 8), F32)

    def pack_step(k, carry):
        for i in range(NV):
            pieces = []
            for p in range(2):
                for z in range(2):
                    pieces += [coarse_b[k, p, i, z], gap]
            packed[k, i] = jnp.concatenate(pieces, axis=-1)
        return carry

    lax.fori_loop(0, 9, pack_step, 0)
    loads[5].wait()
    rrow[...] = jnp.zeros_like(rrow)
    for copy in first:
        copy.wait_recv()
    fine_outer(iterate, 0, res, True)

    row2 = lax.broadcasted_iota(jnp.int32, (8, 128), 0)
    lane2 = lax.broadcasted_iota(jnp.int32, (8, 128), 1)
    spread = (lane2 % 32 // 4 == row2).astype(F32)

    def round_step(s, carry):
        for z in range(2):
            re = wide[z, 0, s].astype(jnp.bfloat16)
            im = wide[z, 1, s].astype(jnp.bfloat16)
            field[z, 0, s] = re
            field[z, 1, s] = im
            field[z, 2, s] = -re
        return carry

    lax.fori_loop(0, 12, round_step, 0)

    def running(total, a, b):
        product = a.astype(F32) * b.astype(F32)
        return product if total is None else total + product

    for z in range(2):
        slot = slot_ref[z]

        def restrict_step(i, carry):
            for j in range(2):
                first_v = 4 * i + 2 * j
                totals = [[None, None], [None, None]]
                for s in range(12):
                    for u in range(2):
                        nr = null_b[slot, 0, first_v + u, s]
                        ni = null_b[slot, 1, first_v + u, s]
                        totals[u][0] = running(totals[u][0], nr, field[z, 0, s])
                        totals[u][1] = running(totals[u][1], nr, field[z, 1, s])
                        totals[u][0] = running(totals[u][0], ni, field[z, 1, s])
                        totals[u][1] = running(totals[u][1], ni, field[z, 2, s])
                for u in range(2):
                    for q in range(2):
                        rrow[pl.ds(64 * q + 32 * z + first_v + u, 1)] = jnp.sum(totals[u][q], axis=0, keepdims=True)
            return carry

        lax.fori_loop(0, NV // 4, restrict_step, 0)

    rhs = lax.dot_general(
        spread, rrow[...], (((1,), (1,)), ((), ())), precision=HIGHEST, preferred_element_type=F32
    )
    w = RELAX_WEIGHT * rhs
    lower_z = lane2 % 64 < 32
    lower_p = lane2 < 64
    parity = jnp.where(lower_p, 1.0, -1.0)

    def accumulate(sums, k, vector):
        blocks = packed[k]
        re = blocks * (vector * parity)[None]
        im = blocks * pltpu.roll(vector, 64, 1)[None]
        return (re, im) if sums is None else (sums[0] + re, sums[1] + im)

    def folded(low, high, distance):
        lanes = lax.broadcasted_iota(jnp.int32, low.shape, low.ndim - 1)
        clear = lanes // distance % 2 == 0
        axis = low.ndim - 1
        return jnp.where(clear, low, pltpu.roll(high, distance, axis)) + jnp.where(
            clear, pltpu.roll(low, 128 - distance, axis), high
        )

    sent = []
    for iteration in range(3):
        wbuf[iteration] = w
        phase = 1 + iteration
        copies = [
            remote(phase, d, wbuf.at[iteration], c_halo.at[iteration, d]) for d in range(6)
        ]
        for copy in copies:
            copy.start()
        sent += copies
        sums = accumulate(None, 0, w)
        sums = accumulate(sums, 7, pltpu.roll(w, 7, 0))
        sums = accumulate(sums, 8, pltpu.roll(w, 1, 0))
        copies[2].wait_recv()
        copies[3].wait_recv()
        ahead = jnp.where(lower_z, pltpu.roll(w, 96, 1), pltpu.roll(c_halo[iteration, 2], 32, 1))
        sums = accumulate(sums, 3, ahead)
        behind = jnp.where(lower_z, pltpu.roll(c_halo[iteration, 3], 96, 1), pltpu.roll(w, 32, 1))
        sums = accumulate(sums, 4, behind)
        for k, d in ((1, 0), (2, 1), (5, 4), (6, 5)):
            copies[d].wait_recv()
            sums = accumulate(sums, k, c_halo[iteration, d])
        wide_p = lax.broadcasted_iota(jnp.int32, (NV, 8, 128), 2) < 64
        folds = jnp.where(wide_p, sums[0], sums[1]) + pltpu.roll(jnp.where(wide_p, sums[1], sums[0]), 64, 2)
        middle = folds[8:16]
        bit = lax.broadcasted_iota(jnp.int32, (8, 8, 128), 2) // 16 % 2 == 0
        middle = jnp.where(bit, middle + pltpu.roll(middle, 112, 2), 0.0)
        folds = folded(folded(folds[0:8], folds[16:24], 16), middle, 8)
        folds = folded(folds[0:4], folds[4:8], 4)
        folds = folded(folds[0:2], folds[2:4], 2)
        total = folded(folds[0], folds[1], 1)
        w = w + RELAX_WEIGHT * (rhs - (2.0 * w + total))

    coef[...] = jnp.dot(
        jnp.transpose(w.astype(jnp.bfloat16).astype(F32)), spread, preferred_element_type=F32
    )
    def tile_step(v, carry):
        for z in range(2):
            re = jnp.broadcast_to(coef[pl.ds(32 * z + v, 1)], (16, 128))
            im = jnp.broadcast_to(coef[pl.ds(64 + 32 * z + v, 1)], (16, 128))
            for kind, value in enumerate((re, im, -im)):
                tile[z, kind, v] = value.astype(jnp.bfloat16)
        return carry

    lax.fori_loop(0, NV, tile_step, 0)

    for z in range(2):
        slot = slot_ref[z]

        def prolong_step(i, carry):
            totals = [[None, None], [None, None]]
            for v in range(NV):
                for p in range(2):
                    for u in range(2):
                        null = null_b[slot, p, v, 2 * i + u]
                        for q in range(2):
                            kind = ((0, 2), (1, 0))[q][p]
                            totals[u][q] = running(totals[u][q], null, tile[z, kind, v])
            for u in range(2):
                s = 2 * i + u
                spin, colour = s // 3, lax.rem(s, 3)
                for q in range(2):
                    for t in range(4):
                        corr[q, spin, colour, t, 4 * z : 4 * z + 4] = totals[u][q][4 * t : 4 * t + 4]
            return carry

        lax.fori_loop(0, 6, prolong_step, 0)

    second = fine_send(corr, 1)

    def add_step(t, carry):
        out_x[:, :, :, t] = iterate[:, :, :, t] + corr[:, :, :, t]
        return carry

    lax.fori_loop(0, 4, add_step, 0)
    fine_inner(res, corr)
    for copy in second:
        copy.wait_recv()
    fine_outer(corr, 1, out_r, False)
    for copy in first + sent + second:
        copy.wait_send()


def per_device(source, iterate, gauge_links, clover, bc_sign, null_store, block_slot, coarse_links):
    null = null_store.reshape((2, 2, NV, 12, 16, 128))
    coarse = jnp.transpose(coarse_links, (0, 1, 2, 4, 5, 6, 7, 3)).reshape((9, 2, NV, 2, 8, NV))
    slots = block_slot.reshape((2,))
    spinor = pltpu.VMEM((2, 4, 3, 4, 8, 128), F32)
    anywhere = pl.BlockSpec(memory_space=pl.ANY)
    half = (2, 2, 3, 8, 128)
    vmem = lambda *shape: pltpu.VMEM(shape, F32)
    return pl.pallas_call(
        kernel,
        out_shape=(spinor, spinor),
        in_specs=[anywhere] * 8,
        out_specs=(pl.BlockSpec(memory_space=pltpu.VMEM),) * 2,
        scratch_shapes=[
            vmem(*spinor.shape), vmem(*spinor.shape), vmem(4, 2, 3, 3, 4, 8, 128),
            vmem(2, 2, 6, 6, 4, 8, 128), pltpu.VMEM((2, 2, NV, 12, 16, 128), jnp.bfloat16),
            vmem(9, 2, NV, 2, 8, NV), vmem(9, NV, 8, 128),
            vmem(2, 5, *half), vmem(2, 5, *half), vmem(4, *half), vmem(4, *half),
            vmem(2, 4, 2, 2, 3, 1, 128), vmem(2, 4, 2, 2, 3, 1, 128), vmem(2, *half), vmem(2, *half),
            vmem(2, 4, 2, 2, 3, 1, 128), vmem(2, 4, 2, 2, 3, 1, 128), vmem(2, *half), vmem(2, *half),
            vmem(*spinor.shape), vmem(*spinor.shape), vmem(*spinor.shape), vmem(2, 2, 12, 16, 128),
            pltpu.VMEM((2, 3, 12, 16, 128), jnp.bfloat16), vmem(128, 128), vmem(128, 128),
            pltpu.VMEM((2, 3, NV, 16, 128), jnp.bfloat16), vmem(3, 8, 128), vmem(3, 6, 8, 128),
            pltpu.SMEM((4,), jnp.int32), pltpu.SMEM((2,), jnp.int32), pltpu.SemaphoreType.DMA((9,)), pltpu.SemaphoreType.DMA((5, 6)),
            pltpu.SemaphoreType.DMA((5, 6)),
        ],
        compiler_params=pltpu.CompilerParams(
            collective_id=0, has_side_effects=True, vmem_limit_bytes=56 * 1024 * 1024
        ),
    )(source, iterate, gauge_links, clover, null, coarse, bc_sign, slots)


def solution(mesh):
    spinor = P(None, None, None, "ta", "gz", "xy")
    matrix = P(None, None, None, None, "ta", "gz", "xy")
    column = P("ta", "gz", "xy", None, None, None, None, None, None)
    placed = (
        spinor, spinor, matrix, matrix, P(), column, P("ta", "gz", "xy"),
        P(None, None, None, None, "ta", "gz", "xy", None),
    )
    return jax.shard_map(
        per_device, mesh=mesh, in_specs=placed, out_specs=(spinor, spinor), check_vma=False
    )
```

```python
import jax
import jax.numpy as jnp
from jax import lax
from jax.experimental import pallas as pl
from jax.experimental.pallas import tpu as pltpu
from jax.sharding import PartitionSpec as P

MASS_TERM = 3.8
RELAX_WEIGHT = 0.4
NV = 24
HIGHEST = lax.Precision.HIGHEST
MESH = pl.DeviceIdType.MESH
F32 = jnp.float32

UPPER = (((0, 0), (1, 0)), ((0, 3), (1, 1)), ((1, 3), (0, 3)), ((1, 2), (0, 0)))
LOWER = (((0, 0), (1, 0)), ((0, 1), (1, 3)), ((1, 1), (0, 1)), ((1, 0), (0, 2)))


def plus_phase(a, b, power):
    power = power % 4
    if power == 0:
        return (a[0] + b[0], a[1] + b[1])
    if power == 1:
        return (a[0] - b[1], a[1] + b[0])
    if power == 2:
        return (a[0] - b[0], a[1] - b[1])
    return (a[0] + b[1], a[1] - b[0])


def spin_of(ref, spin, t):
    return (ref[0, spin, :, t], ref[1, spin, :, t])


def project(ref, t, mu, sign):
    turn = 0 if sign > 0 else 2
    return [
        plus_phase(spin_of(ref, s, t), spin_of(ref, 2 + UPPER[mu][s][0], t), UPPER[mu][s][1] + turn)
        for s in range(2)
    ]


def times_link(links, mu, t, half):
    out = [None, None]
    for b in range(3):
        ur = links[mu, 0, :, b, t]
        ui = links[mu, 1, :, b, t]
        for s in range(2):
            br = half[s][0][b][None]
            bi = half[s][1][b][None]
            re = ur * br - ui * bi
            im = ur * bi + ui * br
            out[s] = (re, im) if b == 0 else (out[s][0] + re, out[s][1] + im)
    return out


def times_packed(block, half):
    out = [None, None]
    for b in range(3):
        ur = block[0, :, b]
        ui = block[1, :, b]
        for s in range(2):
            br = half[s][0][b][None]
            bi = half[s][1][b][None]
            re = ur * br - ui * bi
            im = ur * bi + ui * br
            out[s] = (re, im) if b == 0 else (out[s][0] + re, out[s][1] + im)
    return out


def times_dagger(links, mu, t, half):
    out = [None, None]
    for b in range(3):
        ur = links[mu, 0, b, :, t]
        ui = links[mu, 1, b, :, t]
        for s in range(2):
            br = half[s][0][b][None]
            bi = half[s][1][b][None]
            re = ur * br + ui * bi
            im = ur * bi - ui * br
            out[s] = (re, im) if b == 0 else (out[s][0] + re, out[s][1] + im)
    return out


def add_hop(total, half, mu, sign):
    turn = 0 if sign > 0 else 2
    if total is None:
        zero = jnp.zeros_like(half[0][0])
        total = [half[0], half[1], (zero, zero), (zero, zero)]
    else:
        total = [
            plus_phase(total[0], half[0], 0),
            plus_phase(total[1], half[1], 0),
            total[2],
            total[3],
        ]
    for s in range(2):
        source, power = LOWER[mu][s]
        total[2 + s] = plus_phase(total[2 + s], half[source], power + turn)
    return total


def each(half, function):
    return [(function(re), function(im)) for re, im in half]


def both(first, second, function):
    return [(function(a[0], b[0]), function(a[1], b[1])) for a, b in zip(first, second)]


def kernel(
    source_h, iterate_h, links_h, clover_h, null_h, coarse_h, bc_h, slot_h,
    out_x, out_r,
    source, iterate, links, clover, null_b, coarse_b, packed,
    ht_s, gt_s, ht_r, gt_r, ux, uz, rz, gz, gx, hz_s, gz_s, hx_s, gx_s, hz_r, gz_r, hx_r, gx_r,
    part, res, corr, wide, field, rrow, coef, tile, wbuf,
    c_halo, bc_ref, slot_ref, local_sem, send_sem, recv_sem,
):
    me = (lax.axis_index("ta"), lax.axis_index("gz"), lax.axis_index("xy"))
    size = (lax.axis_size("ta"), lax.axis_size("gz"), lax.axis_size("xy"))

    def peer(axis, step):
        place = list(me)
        place[axis] = lax.rem(me[axis] + step + size[axis], size[axis])
        return tuple(place)

    loads = [
        pltpu.make_async_copy(source_from, into, local_sem.at[i])
        for i, (source_from, into) in enumerate((
            (iterate_h, iterate), (links_h.at[0:3], links.at[0:3]), (clover_h, clover), (source_h, source),
            (coarse_h, coarse_b), (null_h, null_b), (links_h.at[3], links.at[3]),
            (bc_h, bc_ref), (slot_h, slot_ref),
        ))
    ]
    loads[0].start()
    loads[1].start()
    barrier = pltpu.get_barrier_semaphore()
    for axis in range(3):
        for step in (-1, 1):
            pl.semaphore_signal(barrier, inc=1, device_id=peer(axis, step), device_id_type=MESH)

    lane = lax.broadcasted_iota(jnp.int32, (3, 8, 128), 2)
    row = lax.broadcasted_iota(jnp.int32, (3, 8, 128), 1)
    place_y = lane % 32

    def sign_of(mu, at_edge):
        return jnp.where(at_edge, bc_ref[mu], 1).astype(F32)

    def remote(phase, d, source_from, into):
        return pltpu.make_async_remote_copy(
            src_ref=source_from, dst_ref=into, send_sem=send_sem.at[phase, d],
            recv_sem=recv_sem.at[phase, d],
            device_id=peer(d // 2, -1 if d % 2 == 0 else 1), device_id_type=MESH,
        )

    def store_half(ref, index, half):
        for s in range(2):
            ref[index + (0, s)] = half[s][0]
            ref[index + (1, s)] = half[s][1]

    def load_half(ref, index):
        return [(ref[index + (0, s)], ref[index + (1, s)]) for s in range(2)]

    def fine_copies(n):
        phase = 4 * n
        return [
            remote(phase, 0, ht_s.at[n], ht_r.at[n]),
            remote(phase, 1, gt_s.at[n], gt_r.at[n]),
            remote(phase, 2, hz_s.at[n], hz_r.at[n]),
            remote(phase, 3, gz_s.at[n], gz_r.at[n]),
            remote(phase, 4, hx_s.at[n], hx_r.at[n]),
            remote(phase, 5, gx_s.at[n], gx_r.at[n]),
        ]

    def fine_send(vec, n):
        copies = fine_copies(n)

        def send_x():
            ahead = None
            behind = None
            for t in range(4):
                here = lane // 32 == t
                half = project(vec, t, 2, -1)
                back = times_dagger(links, 2, t, project(vec, t, 2, 1))
                store_half(gx, (t,), back)
                half = each(half, lambda a: pltpu.roll(a, 32 * t, 2) if t else a)
                back = each(back, lambda a: pltpu.roll(a, (32 * t + 32) % 128, 2) if t < 3 else a)
                ahead = half if t == 0 else both(half, ahead, lambda a, b: jnp.where(here, a, b))
                behind = back if t == 0 else both(back, behind, lambda a, b: jnp.where(here, a, b))
            store_half(hx_s, (n,), ahead)
            store_half(gx_s, (n,), behind)

        def step_z(t, carry):
            half = project(vec, t, 1, -1)
            for s in range(2):
                for q in range(2):
                    hz_s[n, q, s, :, t : t + 1, :] = half[s][q][:, 0:1, :]
            back = times_dagger(links, 1, t, project(vec, t, 1, 1))
            store_half(gz, (t,), back)
            store_half(gz_s, (n, t), each(back, lambda a: a[:, 7:8, :]))
            return carry

        store_half(ht_s, (n,), project(vec, 0, 0, -1))
        store_half(gt_s, (n,), times_dagger(links, 0, 3, project(vec, 3, 0, 1)))
        if n == 0:
            pl.semaphore_wait(barrier, 6)
        copies[0].start()
        copies[1].start()
        send_x()
        copies[4].start()
        copies[5].start()
        for t in range(4):
            step_z(t, 0)
        copies[2].start()
        copies[3].start()
        return copies

    def fine_inner(start, vec):
        def step(t, carry):
            half = project(vec, t, 3, -1)
            half = each(half, lambda a: jnp.where(place_y == 31, sign_y * pltpu.roll(a, 31, 2), pltpu.roll(a, 127, 2)))
            total = add_hop(None, times_link(links, 3, t, half), 3, -1)
            back = times_dagger(links, 3, t, project(vec, t, 3, 1))
            back = each(back, lambda a: jnp.where(place_y == 0, sign_y * pltpu.roll(a, 97, 2), pltpu.roll(a, 1, 2)))
            total = add_hop(total, back, 3, 1)
            for chirality in range(2):
                out_re = [None, None]
                out_im = [None, None]
                for column in range(6):
                    spin, colour = 2 * chirality + column // 3, column % 3
                    vr = vec[0, spin, colour, t][None]
                    vi = vec[1, spin, colour, t][None]
                    for s in range(2):
                        mr = clover[chirality, 0, 3 * s : 3 * s + 3, column, t]
                        mi = clover[chirality, 1, 3 * s : 3 * s + 3, column, t]
                        re = mr * vr - mi * vi
                        im = mr * vi + mi * vr
                        out_re[s] = re if column == 0 else out_re[s] + re
                        out_im[s] = im if column == 0 else out_im[s] + im
                for s in range(2):
                    spin = 2 * chirality + s
                    vr, vi = spin_of(vec, spin, t)
                    part[0, spin, :, t] = start[0, spin, :, t] - MASS_TERM * vr - out_re[s] + 0.5 * total[spin][0]
                    part[1, spin, :, t] = start[1, spin, :, t] - MASS_TERM * vi - out_im[s] + 0.5 * total[spin][1]
            return carry

        def add_part(t, total):
            for spin in range(4):
                for q in range(2):
                    part[q, spin, :, t] = part[q, spin, :, t] + 0.5 * total[spin][q]

        def step_zx(t, carry):
            half = each(project(vec, t, 1, -1), lambda a: jnp.where(row == 7, 0.0, pltpu.roll(a, 7, 1)))
            total = add_hop(None, times_link(links, 1, t, half), 1, -1)
            back = each(load_half(gz, (t,)), lambda a: jnp.where(row == 0, 0.0, pltpu.roll(a, 1, 1)))
            total = add_hop(total, back, 1, 1)
            half = each(project(vec, t, 2, -1), lambda a: jnp.where(lane >= 96, 0.0, pltpu.roll(a, 96, 2)))
            total = add_hop(total, times_link(links, 2, t, half), 2, -1)
            back = each(load_half(gx, (t,)), lambda a: jnp.where(lane < 32, 0.0, pltpu.roll(a, 32, 2)))
            add_part(t, add_hop(total, back, 2, 1))
            return carry

        def step_t(t, carry):
            add_part(t, add_hop(None, times_link(links, 0, t, project(vec, t + 1, 0, -1)), 0, -1))
            add_part(t + 1, add_hop(None, times_dagger(links, 0, t, project(vec, t, 0, 1)), 0, 1))
            return carry

        lax.fori_loop(0, 4, step, 0)
        lax.fori_loop(0, 4, step_zx, 0)
        lax.fori_loop(0, 3, step_t, 0)

    def prepare_edges():
        lane9 = lax.broadcasted_iota(jnp.int32, (3, 3, 8, 128), 3)
        for p in range(2):
            gathered = None
            for t in range(4):
                block = links[2, p, :, :, t]
                if t < 3:
                    block = pltpu.roll(block, (32 * t + 32) % 128, 3)
                gathered = block if t == 0 else jnp.where(lane9 // 32 == t, block, gathered)
                uz[p, :, :, t : t + 1, :] = links[1, p, :, :, t, 7:8, :]
            ux[p] = gathered

    def fine_outer(vec, n, out, keep):
        def scaled(half, sign):
            factor = 0.5 * sign
            return each(half, lambda a: a * factor)

        ahead_t = times_link(links, 0, 3, scaled(load_half(ht_r, (n,)), top[0]))
        behind_t = scaled(load_half(gt_r, (n,)), bottom[0])
        ahead_x = times_packed(ux, scaled(load_half(hx_r, (n,)), top[2]))
        behind_x = scaled(load_half(gx_r, (n,)), bottom[2])
        store_half(rz, (), times_packed(uz, scaled(load_half(hz_r, (n,)), top[1])))
        for t in range(4):
            half = each(ahead_x, lambda a: jnp.where(lane >= 96, pltpu.roll(a, 96 - 32 * t, 2) if t < 3 else a, 0.0))
            total = add_hop(None, half, 2, -1)
            half = each(behind_x, lambda a: jnp.where(lane < 32, pltpu.roll(a, 128 - 32 * t, 2) if t else a, 0.0))
            total = add_hop(total, half, 2, 1)
            half = [(rz[0, s, :, t : t + 1, :], rz[1, s, :, t : t + 1, :]) for s in range(2)]
            total = add_hop(total, each(half, lambda a: jnp.where(row == 7, a, 0.0)), 1, -1)
            half = scaled(load_half(gz_r, (n, t)), bottom[1])
            total = add_hop(total, each(half, lambda a: jnp.where(row == 0, a, 0.0)), 1, 1)
            if t == 3:
                total = add_hop(total, ahead_t, 0, -1)
            if t == 0:
                total = add_hop(total, behind_t, 0, 1)
            for spin in range(4):
                for q in range(2):
                    value = part[q, spin, :, t] + total[spin][q]
                    out[q, spin, :, t] = value
                    if keep:
                        for z in range(2):
                            for colour in range(3):
                                wide[z, q, 3 * spin + colour, 4 * t : 4 * t + 4] = value[colour, 4 * z : 4 * z + 4]

    loads[0].wait()
    loads[1].wait()
    for i in (7, 8, 6, 2, 3, 5, 4):
        loads[i].start()
    first = fine_send(iterate, 0)
    for i in (7, 8, 6, 2):
        loads[i].wait()
    loads[3].wait()
    top = [sign_of(axis, me[axis] == size[axis] - 1) for axis in range(3)]
    bottom = [sign_of(axis, me[axis] == 0) for axis in range(3)]
    sign_y = bc_ref[3].astype(F32)
    prepare_edges()
    fine_inner(source, iterate)

    loads[5].wait()
    rrow[...] = jnp.zeros_like(rrow)
    for copy in first:
        copy.wait_recv()
    fine_outer(iterate, 0, res, True)

    row2 = lax.broadcasted_iota(jnp.int32, (8, 128), 0)
    lane2 = lax.broadcasted_iota(jnp.int32, (8, 128), 1)
    spread = (lane2 % 32 // 4 == row2).astype(F32)

    def round_step(s, carry):
        for z in range(2):
            re = wide[z, 0, s].astype(jnp.bfloat16)
            im = wide[z, 1, s].astype(jnp.bfloat16)
            field[z, 0, s] = re
            field[z, 1, s] = im
            field[z, 2, s] = -re
        return carry

    for s in range(12):
        round_step(s, 0)

    def running(total, a, b):
        product = a.astype(F32) * b.astype(F32)
        return product if total is None else total + product

    for z in range(2):
        slot = slot_ref[z]

        def restrict_step(i, carry):
            for j in range(4):
                first_v = 8 * i + 2 * j
                totals = [[None, None], [None, None]]
                for s in range(12):
                    for u in range(2):
                        nr = null_b[slot, 0, first_v + u, s]
                        ni = null_b[slot, 1, first_v + u, s]
                        totals[u][0] = running(totals[u][0], nr, field[z, 0, s])
                        totals[u][1] = running(totals[u][1], nr, field[z, 1, s])
                        totals[u][0] = running(totals[u][0], ni, field[z, 1, s])
                        totals[u][1] = running(totals[u][1], ni, field[z, 2, s])
                for u in range(2):
                    for q in range(2):
                        rrow[pl.ds(64 * q + 32 * z + first_v + u, 1)] = jnp.sum(totals[u][q], axis=0, keepdims=True)
            return carry

        lax.fori_loop(0, NV // 8, restrict_step, 0)

    rhs = lax.dot_general(
        spread, rrow[...], (((1,), (1,)), ((), ())), precision=HIGHEST, preferred_element_type=F32
    )
    w = RELAX_WEIGHT * rhs
    lower_z = lane2 % 64 < 32
    lower_p = lane2 < 64
    parity = jnp.where(lower_p, 1.0, -1.0)

    def accumulate(sums, k, vector):
        blocks = packed[k]
        re = blocks * (vector * parity)[None]
        im = blocks * pltpu.roll(vector, 64, 1)[None]
        return (re, im) if sums is None else (sums[0] + re, sums[1] + im)

    def folded(low, high, distance):
        lanes = lax.broadcasted_iota(jnp.int32, low.shape, low.ndim - 1)
        clear = lanes // distance % 2 == 0
        axis = low.ndim - 1
        return jnp.where(clear, low, pltpu.roll(high, distance, axis)) + jnp.where(
            clear, pltpu.roll(low, 128 - distance, axis), high
        )

    gap = jnp.zeros((8, 8), F32)

    def pack_step(k, carry):
        for i in range(NV):
            pieces = []
            for p in range(2):
                for z in range(2):
                    pieces += [coarse_b[k, p, i, z], gap]
            packed[k, i] = jnp.concatenate(pieces, axis=-1)
        return carry

    sent = []
    for iteration in range(3):
        wbuf[iteration] = w
        phase = 1 + iteration
        copies = [
            remote(phase, d, wbuf.at[iteration], c_halo.at[iteration, d]) for d in range(6)
        ]
        for copy in copies:
            copy.start()
        sent += copies
        if iteration == 0:
            loads[4].wait()
            lax.fori_loop(0, 9, pack_step, 0)
        sums = accumulate(None, 0, w)
        sums = accumulate(sums, 7, pltpu.roll(w, 7, 0))
        sums = accumulate(sums, 8, pltpu.roll(w, 1, 0))
        copies[2].wait_recv()
        copies[3].wait_recv()
        ahead = jnp.where(lower_z, pltpu.roll(w, 96, 1), pltpu.roll(c_halo[iteration, 2], 32, 1))
        sums = accumulate(sums, 3, ahead)
        behind = jnp.where(lower_z, pltpu.roll(c_halo[iteration, 3], 96, 1), pltpu.roll(w, 32, 1))
        sums = accumulate(sums, 4, behind)
        for k, d in ((1, 0), (2, 1), (5, 4), (6, 5)):
            copies[d].wait_recv()
            sums = accumulate(sums, k, c_halo[iteration, d])
        wide_p = lax.broadcasted_iota(jnp.int32, (NV, 8, 128), 2) < 64
        folds = jnp.where(wide_p, sums[0], sums[1]) + pltpu.roll(jnp.where(wide_p, sums[1], sums[0]), 64, 2)
        middle = folds[8:16]
        bit = lax.broadcasted_iota(jnp.int32, (8, 8, 128), 2) // 16 % 2 == 0
        middle = jnp.where(bit, middle + pltpu.roll(middle, 112, 2), 0.0)
        folds = folded(folded(folds[0:8], folds[16:24], 16), middle, 8)
        folds = folded(folds[0:4], folds[4:8], 4)
        folds = folded(folds[0:2], folds[2:4], 2)
        total = folded(folds[0], folds[1], 1)
        w = w + RELAX_WEIGHT * (rhs - (2.0 * w + total))

    coef[...] = jnp.dot(
        jnp.transpose(w.astype(jnp.bfloat16).astype(F32)), spread, preferred_element_type=F32
    )
    def tile_step(v, carry):
        for z in range(2):
            re = jnp.broadcast_to(coef[pl.ds(32 * z + v, 1)], (16, 128))
            im = jnp.broadcast_to(coef[pl.ds(64 + 32 * z + v, 1)], (16, 128))
            for kind, value in enumerate((re, im, -im)):
                tile[z, kind, v] = value.astype(jnp.bfloat16)
        return carry

    for v in range(NV):
        tile_step(v, 0)

    for z in range(2):
        slot = slot_ref[z]

        def prolong_step(i, carry):
            totals = [[None, None], [None, None]]
            for v in range(NV):
                for p in range(2):
                    for u in range(2):
                        null = null_b[slot, p, v, 2 * i + u]
                        for q in range(2):
                            kind = ((0, 2), (1, 0))[q][p]
                            totals[u][q] = running(totals[u][q], null, tile[z, kind, v])
            for u in range(2):
                s = 2 * i + u
                spin, colour = s // 3, lax.rem(s, 3)
                for q in range(2):
                    for t in range(4):
                        corr[q, spin, colour, t, 4 * z : 4 * z + 4] = totals[u][q][4 * t : 4 * t + 4]
            return carry

        def prolong_pair(i, carry):
            prolong_step(2 * i, carry)
            return prolong_step(2 * i + 1, carry)

        lax.fori_loop(0, 3, prolong_pair, 0)

    second = fine_send(corr, 1)

    def add_step(t, carry):
        out_x[:, :, :, t] = iterate[:, :, :, t] + corr[:, :, :, t]
        return carry

    lax.fori_loop(0, 4, add_step, 0)
    fine_inner(res, corr)
    for copy in second:
        copy.wait_recv()
    fine_outer(corr, 1, out_r, False)
    for copy in first + sent + second:
        copy.wait_send()


def per_device(source, iterate, gauge_links, clover, bc_sign, null_store, block_slot, coarse_links):
    null = null_store.reshape((2, 2, NV, 12, 16, 128))
    coarse = jnp.transpose(coarse_links, (0, 1, 2, 4, 5, 6, 7, 3)).reshape((9, 2, NV, 2, 8, NV))
    slots = block_slot.reshape((2,))
    spinor = pltpu.VMEM((2, 4, 3, 4, 8, 128), F32)
    anywhere = pl.BlockSpec(memory_space=pl.ANY)
    half = (2, 2, 3, 8, 128)
    vmem = lambda *shape: pltpu.VMEM(shape, F32)
    return pl.pallas_call(
        kernel,
        out_shape=(spinor, spinor),
        in_specs=[anywhere] * 8,
        out_specs=(pl.BlockSpec(memory_space=pltpu.VMEM),) * 2,
        scratch_shapes=[
            vmem(*spinor.shape), vmem(*spinor.shape), vmem(4, 2, 3, 3, 4, 8, 128),
            vmem(2, 2, 6, 6, 4, 8, 128), pltpu.VMEM((2, 2, NV, 12, 16, 128), jnp.bfloat16),
            vmem(9, 2, NV, 2, 8, NV), vmem(9, NV, 8, 128),
            vmem(2, *half), vmem(2, *half), vmem(2, *half), vmem(2, *half),
            vmem(2, 3, 3, 8, 128), vmem(2, 3, 3, 4, 128), vmem(2, 2, 3, 4, 128), vmem(4, *half), vmem(4, *half),
            vmem(2, 2, 2, 3, 4, 128), vmem(2, 4, 2, 2, 3, 1, 128), vmem(2, *half), vmem(2, *half),
            vmem(2, 2, 2, 3, 4, 128), vmem(2, 4, 2, 2, 3, 1, 128), vmem(2, *half), vmem(2, *half),
            vmem(*spinor.shape), vmem(*spinor.shape), vmem(*spinor.shape), vmem(2, 2, 12, 16, 128),
            pltpu.VMEM((2, 3, 12, 16, 128), jnp.bfloat16), vmem(128, 128), vmem(128, 128),
            pltpu.VMEM((2, 3, NV, 16, 128), jnp.bfloat16), vmem(3, 8, 128), vmem(3, 6, 8, 128),
            pltpu.SMEM((4,), jnp.int32), pltpu.SMEM((2,), jnp.int32), pltpu.SemaphoreType.DMA((9,)), pltpu.SemaphoreType.DMA((5, 6)),
            pltpu.SemaphoreType.DMA((5, 6)),
        ],
        compiler_params=pltpu.CompilerParams(
            collective_id=0, has_side_effects=True, vmem_limit_bytes=56 * 1024 * 1024
        ),
    )(source, iterate, gauge_links, clover, null, coarse, bc_sign, slots)


def solution(mesh):
    spinor = P(None, None, None, "ta", "gz", "xy")
    matrix = P(None, None, None, None, "ta", "gz", "xy")
    column = P("ta", "gz", "xy", None, None, None, None, None, None)
    placed = (
        spinor, spinor, matrix, matrix, P(), column, P("ta", "gz", "xy"),
        P(None, None, None, None, "ta", "gz", "xy", None),
    )
    return jax.shard_map(
        per_device, mesh=mesh, in_specs=placed, out_specs=(spinor, spinor), check_vma=False
    )
```

```python
import jax
import jax.numpy as jnp
from jax import lax
from jax.experimental import pallas as pl
from jax.experimental.pallas import tpu as pltpu
from jax.sharding import PartitionSpec as P

MASS_TERM = 3.8
RELAX_WEIGHT = 0.4
NV = 24
HIGHEST = lax.Precision.HIGHEST
MESH = pl.DeviceIdType.MESH
F32 = jnp.float32

UPPER = (((0, 0), (1, 0)), ((0, 3), (1, 1)), ((1, 3), (0, 3)), ((1, 2), (0, 0)))
LOWER = (((0, 0), (1, 0)), ((0, 1), (1, 3)), ((1, 1), (0, 1)), ((1, 0), (0, 2)))


def plus_phase(a, b, power):
    power = power % 4
    if power == 0:
        return (a[0] + b[0], a[1] + b[1])
    if power == 1:
        return (a[0] - b[1], a[1] + b[0])
    if power == 2:
        return (a[0] - b[0], a[1] - b[1])
    return (a[0] + b[1], a[1] - b[0])


def spin_of(ref, spin, t):
    return (ref[0, spin, :, t], ref[1, spin, :, t])


def project(ref, t, mu, sign):
    turn = 0 if sign > 0 else 2
    return [
        plus_phase(spin_of(ref, s, t), spin_of(ref, 2 + UPPER[mu][s][0], t), UPPER[mu][s][1] + turn)
        for s in range(2)
    ]


def times_link(links, mu, t, half):
    out = [None, None]
    for b in range(3):
        ur = links[mu, 0, :, b, t]
        ui = links[mu, 1, :, b, t]
        for s in range(2):
            br = half[s][0][b][None]
            bi = half[s][1][b][None]
            re = ur * br - ui * bi
            im = ur * bi + ui * br
            out[s] = (re, im) if b == 0 else (out[s][0] + re, out[s][1] + im)
    return out


def times_packed(block, half):
    out = [None, None]
    for b in range(3):
        ur = block[0, :, b]
        ui = block[1, :, b]
        for s in range(2):
            br = half[s][0][b][None]
            bi = half[s][1][b][None]
            re = ur * br - ui * bi
            im = ur * bi + ui * br
            out[s] = (re, im) if b == 0 else (out[s][0] + re, out[s][1] + im)
    return out


def times_dagger(links, mu, t, half):
    out = [None, None]
    for b in range(3):
        ur = links[mu, 0, b, :, t]
        ui = links[mu, 1, b, :, t]
        for s in range(2):
            br = half[s][0][b][None]
            bi = half[s][1][b][None]
            re = ur * br + ui * bi
            im = ur * bi - ui * br
            out[s] = (re, im) if b == 0 else (out[s][0] + re, out[s][1] + im)
    return out


def add_hop(total, half, mu, sign):
    turn = 0 if sign > 0 else 2
    if total is None:
        zero = jnp.zeros_like(half[0][0])
        total = [half[0], half[1], (zero, zero), (zero, zero)]
    else:
        total = [
            plus_phase(total[0], half[0], 0),
            plus_phase(total[1], half[1], 0),
            total[2],
            total[3],
        ]
    for s in range(2):
        source, power = LOWER[mu][s]
        total[2 + s] = plus_phase(total[2 + s], half[source], power + turn)
    return total


def each(half, function):
    return [(function(re), function(im)) for re, im in half]


def both(first, second, function):
    return [(function(a[0], b[0]), function(a[1], b[1])) for a, b in zip(first, second)]


def kernel(
    source_h, iterate_h, links_h, clover_h, null_h, coarse_h, bc_h, slot_h,
    out_x, out_r,
    source, iterate, links, clover, null_b, coarse_b, packed,
    ht_s, gt_s, ht_r, gt_r, ux, uz, rz, gz, gx, hz_s, gz_s, hx_s, gx_s, hz_r, gz_r, hx_r, gx_r,
    part, res, corr, wide, field, rrow, coef, tile, wbuf,
    c_halo, bc_ref, slot_ref, local_sem, send_sem, recv_sem,
):
    me = (lax.axis_index("ta"), lax.axis_index("gz"), lax.axis_index("xy"))
    size = (lax.axis_size("ta"), lax.axis_size("gz"), lax.axis_size("xy"))

    def peer(axis, step):
        place = list(me)
        place[axis] = lax.rem(me[axis] + step + size[axis], size[axis])
        return tuple(place)

    loads = [
        pltpu.make_async_copy(source_from, into, local_sem.at[i])
        for i, (source_from, into) in enumerate((
            (iterate_h, iterate), (links_h.at[0], links.at[0]), (clover_h, clover), (source_h, source),
            (coarse_h, coarse_b), (null_h, null_b), (links_h.at[3], links.at[3]),
            (bc_h, bc_ref), (slot_h, slot_ref), (links_h.at[2], links.at[2]), (links_h.at[1], links.at[1]),
        ))
    ]
    for i in (0, 1, 9, 10):
        loads[i].start()
    barrier = pltpu.get_barrier_semaphore()
    for axis in range(3):
        for step in (-1, 1):
            pl.semaphore_signal(barrier, inc=1, device_id=peer(axis, step), device_id_type=MESH)

    lane = lax.broadcasted_iota(jnp.int32, (3, 8, 128), 2)
    row = lax.broadcasted_iota(jnp.int32, (3, 8, 128), 1)
    place_y = lane % 32

    def sign_of(mu, at_edge):
        return jnp.where(at_edge, bc_ref[mu], 1).astype(F32)

    def remote(phase, d, source_from, into):
        return pltpu.make_async_remote_copy(
            src_ref=source_from, dst_ref=into, send_sem=send_sem.at[phase, d],
            recv_sem=recv_sem.at[phase, d],
            device_id=peer(d // 2, -1 if d % 2 == 0 else 1), device_id_type=MESH,
        )

    def store_half(ref, index, half):
        for s in range(2):
            ref[index + (0, s)] = half[s][0]
            ref[index + (1, s)] = half[s][1]

    def load_half(ref, index):
        return [(ref[index + (0, s)], ref[index + (1, s)]) for s in range(2)]

    def fine_copies(n):
        phase = 4 * n
        return [
            remote(phase, 0, ht_s.at[n], ht_r.at[n]),
            remote(phase, 1, gt_s.at[n], gt_r.at[n]),
            remote(phase, 2, hz_s.at[n], hz_r.at[n]),
            remote(phase, 3, gz_s.at[n], gz_r.at[n]),
            remote(phase, 4, hx_s.at[n], hx_r.at[n]),
            remote(phase, 5, gx_s.at[n], gx_r.at[n]),
        ]

    def fine_send(vec, n):
        copies = fine_copies(n)

        def send_x():
            ahead = None
            behind = None
            for t in range(4):
                here = lane // 32 == t
                half = project(vec, t, 2, -1)
                back = times_dagger(links, 2, t, project(vec, t, 2, 1))
                store_half(gx, (t,), back)
                half = each(half, lambda a: pltpu.roll(a, 32 * t, 2) if t else a)
                back = each(back, lambda a: pltpu.roll(a, (32 * t + 32) % 128, 2) if t < 3 else a)
                ahead = half if t == 0 else both(half, ahead, lambda a, b: jnp.where(here, a, b))
                behind = back if t == 0 else both(back, behind, lambda a, b: jnp.where(here, a, b))
            store_half(hx_s, (n,), ahead)
            store_half(gx_s, (n,), behind)

        def step_z(t, carry):
            half = project(vec, t, 1, -1)
            for s in range(2):
                for q in range(2):
                    hz_s[n, q, s, :, t : t + 1, :] = half[s][q][:, 0:1, :]
            back = times_dagger(links, 1, t, project(vec, t, 1, 1))
            store_half(gz, (t,), back)
            store_half(gz_s, (n, t), each(back, lambda a: a[:, 7:8, :]))
            return carry

        store_half(ht_s, (n,), project(vec, 0, 0, -1))
        store_half(gt_s, (n,), times_dagger(links, 0, 3, project(vec, 3, 0, 1)))
        if n == 0:
            pl.semaphore_wait(barrier, 6)
        copies[0].start()
        copies[1].start()
        if n == 0:
            loads[9].wait()
            for i in (7, 8, 6, 2, 3, 5, 4):
                loads[i].start()
        send_x()
        copies[4].start()
        copies[5].start()
        if n == 0:
            loads[10].wait()
        for t in range(4):
            step_z(t, 0)
        copies[2].start()
        copies[3].start()
        return copies

    def fine_inner(start, vec):
        def step(t, carry):
            half = project(vec, t, 3, -1)
            half = each(half, lambda a: jnp.where(place_y == 31, sign_y * pltpu.roll(a, 31, 2), pltpu.roll(a, 127, 2)))
            total = add_hop(None, times_link(links, 3, t, half), 3, -1)
            back = times_dagger(links, 3, t, project(vec, t, 3, 1))
            back = each(back, lambda a: jnp.where(place_y == 0, sign_y * pltpu.roll(a, 97, 2), pltpu.roll(a, 1, 2)))
            total = add_hop(total, back, 3, 1)
            for chirality in range(2):
                out_re = [None, None]
                out_im = [None, None]
                for column in range(6):
                    spin, colour = 2 * chirality + column // 3, column % 3
                    vr = vec[0, spin, colour, t][None]
                    vi = vec[1, spin, colour, t][None]
                    for s in range(2):
                        mr = clover[chirality, 0, 3 * s : 3 * s + 3, column, t]
                        mi = clover[chirality, 1, 3 * s : 3 * s + 3, column, t]
                        re = mr * vr - mi * vi
                        im = mr * vi + mi * vr
                        out_re[s] = re if column == 0 else out_re[s] + re
                        out_im[s] = im if column == 0 else out_im[s] + im
                for s in range(2):
                    spin = 2 * chirality + s
                    vr, vi = spin_of(vec, spin, t)
                    part[0, spin, :, t] = start[0, spin, :, t] - MASS_TERM * vr - out_re[s] + 0.5 * total[spin][0]
                    part[1, spin, :, t] = start[1, spin, :, t] - MASS_TERM * vi - out_im[s] + 0.5 * total[spin][1]
            return carry

        def add_part(t, total):
            for spin in range(4):
                for q in range(2):
                    part[q, spin, :, t] = part[q, spin, :, t] + 0.5 * total[spin][q]

        def step_zx(t, carry):
            half = each(project(vec, t, 1, -1), lambda a: jnp.where(row == 7, 0.0, pltpu.roll(a, 7, 1)))
            total = add_hop(None, times_link(links, 1, t, half), 1, -1)
            back = each(load_half(gz, (t,)), lambda a: jnp.where(row == 0, 0.0, pltpu.roll(a, 1, 1)))
            total = add_hop(total, back, 1, 1)
            half = each(project(vec, t, 2, -1), lambda a: jnp.where(lane >= 96, 0.0, pltpu.roll(a, 96, 2)))
            total = add_hop(total, times_link(links, 2, t, half), 2, -1)
            back = each(load_half(gx, (t,)), lambda a: jnp.where(lane < 32, 0.0, pltpu.roll(a, 32, 2)))
            add_part(t, add_hop(total, back, 2, 1))
            return carry

        def step_t(t, carry):
            add_part(t, add_hop(None, times_link(links, 0, t, project(vec, t + 1, 0, -1)), 0, -1))
            add_part(t + 1, add_hop(None, times_dagger(links, 0, t, project(vec, t, 0, 1)), 0, 1))
            return carry

        lax.fori_loop(0, 4, step, 0)
        lax.fori_loop(0, 4, step_zx, 0)
        lax.fori_loop(0, 3, step_t, 0)

    def prepare_edges():
        lane9 = lax.broadcasted_iota(jnp.int32, (3, 3, 8, 128), 3)
        for p in range(2):
            gathered = None
            for t in range(4):
                block = links[2, p, :, :, t]
                if t < 3:
                    block = pltpu.roll(block, (32 * t + 32) % 128, 3)
                gathered = block if t == 0 else jnp.where(lane9 // 32 == t, block, gathered)
                uz[p, :, :, t : t + 1, :] = links[1, p, :, :, t, 7:8, :]
            ux[p] = gathered

    def fine_outer(vec, n, out, keep):
        def scaled(half, sign):
            factor = 0.5 * sign
            return each(half, lambda a: a * factor)

        ahead_t = times_link(links, 0, 3, scaled(load_half(ht_r, (n,)), top[0]))
        behind_t = scaled(load_half(gt_r, (n,)), bottom[0])
        ahead_x = times_packed(ux, scaled(load_half(hx_r, (n,)), top[2]))
        behind_x = scaled(load_half(gx_r, (n,)), bottom[2])
        store_half(rz, (), times_packed(uz, scaled(load_half(hz_r, (n,)), top[1])))
        for t in range(4):
            half = each(ahead_x, lambda a: jnp.where(lane >= 96, pltpu.roll(a, 96 - 32 * t, 2) if t < 3 else a, 0.0))
            total = add_hop(None, half, 2, -1)
            half = each(behind_x, lambda a: jnp.where(lane < 32, pltpu.roll(a, 128 - 32 * t, 2) if t else a, 0.0))
            total = add_hop(total, half, 2, 1)
            half = [(rz[0, s, :, t : t + 1, :], rz[1, s, :, t : t + 1, :]) for s in range(2)]
            total = add_hop(total, each(half, lambda a: jnp.where(row == 7, a, 0.0)), 1, -1)
            half = scaled(load_half(gz_r, (n, t)), bottom[1])
            total = add_hop(total, each(half, lambda a: jnp.where(row == 0, a, 0.0)), 1, 1)
            if t == 3:
                total = add_hop(total, ahead_t, 0, -1)
            if t == 0:
                total = add_hop(total, behind_t, 0, 1)
            for spin in range(4):
                for q in range(2):
                    value = part[q, spin, :, t] + total[spin][q]
                    out[q, spin, :, t] = value
                    if keep:
                        for z in range(2):
                            for colour in range(3):
                                wide[z, q, 3 * spin + colour, 4 * t : 4 * t + 4] = value[colour, 4 * z : 4 * z + 4]

    loads[0].wait()
    loads[1].wait()
    first = fine_send(iterate, 0)
    for i in (7, 8, 6, 2):
        loads[i].wait()
    loads[3].wait()
    top = [sign_of(axis, me[axis] == size[axis] - 1) for axis in range(3)]
    bottom = [sign_of(axis, me[axis] == 0) for axis in range(3)]
    sign_y = bc_ref[3].astype(F32)
    prepare_edges()
    fine_inner(source, iterate)

    loads[5].wait()
    rrow[...] = jnp.zeros_like(rrow)
    for copy in first:
        copy.wait_recv()
    fine_outer(iterate, 0, res, True)

    row2 = lax.broadcasted_iota(jnp.int32, (8, 128), 0)
    lane2 = lax.broadcasted_iota(jnp.int32, (8, 128), 1)
    spread = (lane2 % 32 // 4 == row2).astype(F32)

    def round_step(s, carry):
        for z in range(2):
            re = wide[z, 0, s].astype(jnp.bfloat16)
            im = wide[z, 1, s].astype(jnp.bfloat16)
            field[z, 0, s] = re
            field[z, 1, s] = im
            field[z, 2, s] = -re
        return carry

    for s in range(12):
        round_step(s, 0)

    def running(total, a, b):
        product = a.astype(F32) * b.astype(F32)
        return product if total is None else total + product

    for z in range(2):
        slot = slot_ref[z]

        def restrict_step(i, carry):
            for j in range(4):
                first_v = 8 * i + 2 * j
                totals = [[None, None], [None, None]]
                for s in range(12):
                    for u in range(2):
                        nr = null_b[slot, 0, first_v + u, s]
                        ni = null_b[slot, 1, first_v + u, s]
                        totals[u][0] = running(totals[u][0], nr, field[z, 0, s])
                        totals[u][1] = running(totals[u][1], nr, field[z, 1, s])
                        totals[u][0] = running(totals[u][0], ni, field[z, 1, s])
                        totals[u][1] = running(totals[u][1], ni, field[z, 2, s])
                for u in range(2):
                    for q in range(2):
                        rrow[pl.ds(64 * q + 32 * z + first_v + u, 1)] = jnp.sum(totals[u][q], axis=0, keepdims=True)
            return carry

        lax.fori_loop(0, NV // 8, restrict_step, 0)

    rhs = lax.dot_general(
        spread, rrow[...], (((1,), (1,)), ((), ())), precision=HIGHEST, preferred_element_type=F32
    )
    w = RELAX_WEIGHT * rhs
    lower_z = lane2 % 64 < 32
    lower_p = lane2 < 64
    parity = jnp.where(lower_p, 1.0, -1.0)

    def accumulate(sums, k, vector):
        blocks = packed[k]
        re = blocks * (vector * parity)[None]
        im = blocks * pltpu.roll(vector, 64, 1)[None]
        return (re, im) if sums is None else (sums[0] + re, sums[1] + im)

    def folded(low, high, distance):
        lanes = lax.broadcasted_iota(jnp.int32, low.shape, low.ndim - 1)
        clear = lanes // distance % 2 == 0
        axis = low.ndim - 1
        return jnp.where(clear, low, pltpu.roll(high, distance, axis)) + jnp.where(
            clear, pltpu.roll(low, 128 - distance, axis), high
        )

    gap = jnp.zeros((8, 8), F32)

    def pack_step(k, carry):
        for i in range(NV):
            pieces = []
            for p in range(2):
                for z in range(2):
                    pieces += [coarse_b[k, p, i, z], gap]
            packed[k, i] = jnp.concatenate(pieces, axis=-1)
        return carry

    sent = []
    for iteration in range(3):
        wbuf[iteration] = w
        phase = 1 + iteration
        copies = [
            remote(phase, d, wbuf.at[iteration], c_halo.at[iteration, d]) for d in range(6)
        ]
        for copy in copies:
            copy.start()
        sent += copies
        if iteration == 0:
            loads[4].wait()
            lax.fori_loop(0, 9, pack_step, 0)
        sums = accumulate(None, 0, w)
        sums = accumulate(sums, 7, pltpu.roll(w, 7, 0))
        sums = accumulate(sums, 8, pltpu.roll(w, 1, 0))
        copies[2].wait_recv()
        copies[3].wait_recv()
        ahead = jnp.where(lower_z, pltpu.roll(w, 96, 1), pltpu.roll(c_halo[iteration, 2], 32, 1))
        sums = accumulate(sums, 3, ahead)
        behind = jnp.where(lower_z, pltpu.roll(c_halo[iteration, 3], 96, 1), pltpu.roll(w, 32, 1))
        sums = accumulate(sums, 4, behind)
        for k, d in ((1, 0), (2, 1), (5, 4), (6, 5)):
            copies[d].wait_recv()
            sums = accumulate(sums, k, c_halo[iteration, d])
        wide_p = lax.broadcasted_iota(jnp.int32, (NV, 8, 128), 2) < 64
        folds = jnp.where(wide_p, sums[0], sums[1]) + pltpu.roll(jnp.where(wide_p, sums[1], sums[0]), 64, 2)
        middle = folds[8:16]
        bit = lax.broadcasted_iota(jnp.int32, (8, 8, 128), 2) // 16 % 2 == 0
        middle = jnp.where(bit, middle + pltpu.roll(middle, 112, 2), 0.0)
        folds = folded(folded(folds[0:8], folds[16:24], 16), middle, 8)
        folds = folded(folds[0:4], folds[4:8], 4)
        folds = folded(folds[0:2], folds[2:4], 2)
        total = folded(folds[0], folds[1], 1)
        w = w + RELAX_WEIGHT * (rhs - (2.0 * w + total))

    coef[...] = jnp.dot(
        jnp.transpose(w.astype(jnp.bfloat16).astype(F32)), spread, preferred_element_type=F32
    )
    def tile_step(v, carry):
        for z in range(2):
            re = jnp.broadcast_to(coef[pl.ds(32 * z + v, 1)], (16, 128))
            im = jnp.broadcast_to(coef[pl.ds(64 + 32 * z + v, 1)], (16, 128))
            for kind, value in enumerate((re, im, -im)):
                tile[z, kind, v] = value.astype(jnp.bfloat16)
        return carry

    for v in range(NV):
        tile_step(v, 0)

    for z in range(2):
        slot = slot_ref[z]

        def prolong_step(i, carry):
            totals = [[None, None], [None, None]]
            for v in range(NV):
                for p in range(2):
                    for u in range(2):
                        null = null_b[slot, p, v, 2 * i + u]
                        for q in range(2):
                            kind = ((0, 2), (1, 0))[q][p]
                            totals[u][q] = running(totals[u][q], null, tile[z, kind, v])
            for u in range(2):
                s = 2 * i + u
                spin, colour = s // 3, lax.rem(s, 3)
                for q in range(2):
                    for t in range(4):
                        corr[q, spin, colour, t, 4 * z : 4 * z + 4] = totals[u][q][4 * t : 4 * t + 4]
            return carry

        def prolong_pair(i, carry):
            prolong_step(2 * i, carry)
            return prolong_step(2 * i + 1, carry)

        lax.fori_loop(0, 3, prolong_pair, 0)

    second = fine_send(corr, 1)

    def add_step(t, carry):
        out_x[:, :, :, t] = iterate[:, :, :, t] + corr[:, :, :, t]
        return carry

    lax.fori_loop(0, 4, add_step, 0)
    fine_inner(res, corr)
    for copy in second:
        copy.wait_recv()
    fine_outer(corr, 1, out_r, False)
    for copy in first + sent + second:
        copy.wait_send()


def copy_out(x_v, r_v, x_h, r_h, sem):
    copies = [pltpu.make_async_copy(x_v, x_h, sem.at[0]), pltpu.make_async_copy(r_v, r_h, sem.at[1])]
    for copy in copies:
        copy.start()
    for copy in copies:
        copy.wait()


def per_device(source, iterate, gauge_links, clover, bc_sign, null_store, block_slot, coarse_links):
    null = null_store.reshape((2, 2, NV, 12, 16, 128))
    coarse = jnp.transpose(coarse_links, (0, 1, 2, 4, 5, 6, 7, 3)).reshape((9, 2, NV, 2, 8, NV))
    slots = block_slot.reshape((2,))
    spinor = pltpu.VMEM((2, 4, 3, 4, 8, 128), F32)
    anywhere = pl.BlockSpec(memory_space=pl.ANY)
    half = (2, 2, 3, 8, 128)
    vmem = lambda *shape: pltpu.VMEM(shape, F32)
    held = pl.pallas_call(
        kernel,
        out_shape=(spinor, spinor),
        in_specs=[anywhere] * 8,
        out_specs=(pl.BlockSpec(memory_space=pltpu.VMEM),) * 2,
        scratch_shapes=[
            vmem(*spinor.shape), vmem(*spinor.shape), vmem(4, 2, 3, 3, 4, 8, 128),
            vmem(2, 2, 6, 6, 4, 8, 128), pltpu.VMEM((2, 2, NV, 12, 16, 128), jnp.bfloat16),
            vmem(9, 2, NV, 2, 8, NV), vmem(9, NV, 8, 128),
            vmem(2, *half), vmem(2, *half), vmem(2, *half), vmem(2, *half),
            vmem(2, 3, 3, 8, 128), vmem(2, 3, 3, 4, 128), vmem(2, 2, 3, 4, 128), vmem(4, *half), vmem(4, *half),
            vmem(2, 2, 2, 3, 4, 128), vmem(2, 4, 2, 2, 3, 1, 128), vmem(2, *half), vmem(2, *half),
            vmem(2, 2, 2, 3, 4, 128), vmem(2, 4, 2, 2, 3, 1, 128), vmem(2, *half), vmem(2, *half),
            vmem(*spinor.shape), vmem(*spinor.shape), vmem(*spinor.shape), vmem(2, 2, 12, 16, 128),
            pltpu.VMEM((2, 3, 12, 16, 128), jnp.bfloat16), vmem(128, 128), vmem(128, 128),
            pltpu.VMEM((2, 3, NV, 16, 128), jnp.bfloat16), vmem(3, 8, 128), vmem(3, 6, 8, 128),
            pltpu.SMEM((4,), jnp.int32), pltpu.SMEM((2,), jnp.int32), pltpu.SemaphoreType.DMA((11,)), pltpu.SemaphoreType.DMA((5, 6)),
            pltpu.SemaphoreType.DMA((5, 6)),
        ],
        compiler_params=pltpu.CompilerParams(
            collective_id=0, has_side_effects=True, vmem_limit_bytes=56 * 1024 * 1024
        ),
    )(source, iterate, gauge_links, clover, null, coarse, bc_sign, slots)
    held = [pltpu.with_memory_space_constraint(x, pltpu.VMEM) for x in held]
    final = jax.ShapeDtypeStruct(spinor.shape, F32)
    return pl.pallas_call(
        copy_out,
        out_shape=(final, final),
        in_specs=[pl.BlockSpec(memory_space=pltpu.VMEM)] * 2,
        out_specs=(anywhere, anywhere),
        scratch_shapes=[pltpu.SemaphoreType.DMA((2,))],
    )(*held)


def solution(mesh):
    spinor = P(None, None, None, "ta", "gz", "xy")
    matrix = P(None, None, None, None, "ta", "gz", "xy")
    column = P("ta", "gz", "xy", None, None, None, None, None, None)
    placed = (
        spinor, spinor, matrix, matrix, P(), column, P("ta", "gz", "xy"),
        P(None, None, None, None, "ta", "gz", "xy", None),
    )
    return jax.shard_map(
        per_device, mesh=mesh, in_specs=placed, out_specs=(spinor, spinor), check_vma=False
    )
```

```python
import jax
import jax.numpy as jnp
from jax import lax
from jax.experimental import pallas as pl
from jax.experimental.pallas import tpu as pltpu
from jax.sharding import PartitionSpec as P

MASS_TERM = 3.8
RELAX_WEIGHT = 0.4
NV = 24
HIGHEST = lax.Precision.HIGHEST
MESH = pl.DeviceIdType.MESH
F32 = jnp.float32

UPPER = (((0, 0), (1, 0)), ((0, 3), (1, 1)), ((1, 3), (0, 3)), ((1, 2), (0, 0)))
LOWER = (((0, 0), (1, 0)), ((0, 1), (1, 3)), ((1, 1), (0, 1)), ((1, 0), (0, 2)))


def plus_phase(a, b, power):
    power = power % 4
    if power == 0:
        return (a[0] + b[0], a[1] + b[1])
    if power == 1:
        return (a[0] - b[1], a[1] + b[0])
    if power == 2:
        return (a[0] - b[0], a[1] - b[1])
    return (a[0] + b[1], a[1] - b[0])


def spin_of(ref, spin, t):
    return (ref[0, spin, :, t], ref[1, spin, :, t])


def project(ref, t, mu, sign):
    turn = 0 if sign > 0 else 2
    return [
        plus_phase(spin_of(ref, s, t), spin_of(ref, 2 + UPPER[mu][s][0], t), UPPER[mu][s][1] + turn)
        for s in range(2)
    ]


def times_link(links, mu, t, half):
    out = [None, None]
    for b in range(3):
        ur = links[mu, 0, :, b, t]
        ui = links[mu, 1, :, b, t]
        for s in range(2):
            br = half[s][0][b][None]
            bi = half[s][1][b][None]
            re = ur * br - ui * bi
            im = ur * bi + ui * br
            out[s] = (re, im) if b == 0 else (out[s][0] + re, out[s][1] + im)
    return out


def times_packed(block, half):
    out = [None, None]
    for b in range(3):
        ur = block[0, :, b]
        ui = block[1, :, b]
        for s in range(2):
            br = half[s][0][b][None]
            bi = half[s][1][b][None]
            re = ur * br - ui * bi
            im = ur * bi + ui * br
            out[s] = (re, im) if b == 0 else (out[s][0] + re, out[s][1] + im)
    return out


def times_dagger(links, mu, t, half):
    out = [None, None]
    for b in range(3):
        ur = links[mu, 0, b, :, t]
        ui = links[mu, 1, b, :, t]
        for s in range(2):
            br = half[s][0][b][None]
            bi = half[s][1][b][None]
            re = ur * br + ui * bi
            im = ur * bi - ui * br
            out[s] = (re, im) if b == 0 else (out[s][0] + re, out[s][1] + im)
    return out


def add_hop(total, half, mu, sign):
    turn = 0 if sign > 0 else 2
    if total is None:
        zero = jnp.zeros_like(half[0][0])
        total = [half[0], half[1], (zero, zero), (zero, zero)]
    else:
        total = [
            plus_phase(total[0], half[0], 0),
            plus_phase(total[1], half[1], 0),
            total[2],
            total[3],
        ]
    for s in range(2):
        source, power = LOWER[mu][s]
        total[2 + s] = plus_phase(total[2 + s], half[source], power + turn)
    return total


def each(half, function):
    return [(function(re), function(im)) for re, im in half]


def both(first, second, function):
    return [(function(a[0], b[0]), function(a[1], b[1])) for a, b in zip(first, second)]


def kernel(
    source_h, iterate_h, links_h, clover_h, null_h, coarse_h, bc_h, slot_h,
    out_x, out_r,
    source, iterate, links, clover, null_b, coarse_b, packed,
    ht_s, gt_s, ht_r, gt_r, ux, uz, rz, gz, gx, hz_s, gz_s, hx_s, gx_s, hz_r, gz_r, hx_r, gx_r,
    part, res, corr, wide, field, rrow, coef, tile, wbuf,
    c_halo, bc_ref, slot_ref, local_sem, send_sem, recv_sem,
):
    me = (lax.axis_index("ta"), lax.axis_index("gz"), lax.axis_index("xy"))
    size = (lax.axis_size("ta"), lax.axis_size("gz"), lax.axis_size("xy"))

    def peer(axis, step):
        place = list(me)
        place[axis] = lax.rem(me[axis] + step + size[axis], size[axis])
        return tuple(place)

    loads = [
        pltpu.make_async_copy(source_from, into, local_sem.at[i])
        for i, (source_from, into) in enumerate((
            (iterate_h, iterate), (links_h.at[0], links.at[0]), (clover_h, clover), (source_h, source),
            (coarse_h, coarse_b), (null_h, null_b), (links_h.at[3], links.at[3]),
            (bc_h, bc_ref), (slot_h, slot_ref), (links_h.at[2], links.at[2]), (links_h.at[1], links.at[1]),
        ))
    ]
    for i in (0, 1, 9, 10):
        loads[i].start()
    barrier = pltpu.get_barrier_semaphore()
    for axis in range(3):
        for step in (-1, 1):
            pl.semaphore_signal(barrier, inc=1, device_id=peer(axis, step), device_id_type=MESH)

    lane = lax.broadcasted_iota(jnp.int32, (3, 8, 128), 2)
    row = lax.broadcasted_iota(jnp.int32, (3, 8, 128), 1)
    place_y = lane % 32

    def sign_of(mu, at_edge):
        return jnp.where(at_edge, bc_ref[mu], 1).astype(F32)

    def remote(phase, d, source_from, into):
        return pltpu.make_async_remote_copy(
            src_ref=source_from, dst_ref=into, send_sem=send_sem.at[phase, d],
            recv_sem=recv_sem.at[phase, d],
            device_id=peer(d // 2, -1 if d % 2 == 0 else 1), device_id_type=MESH,
        )

    def store_half(ref, index, half):
        for s in range(2):
            ref[index + (0, s)] = half[s][0]
            ref[index + (1, s)] = half[s][1]

    def load_half(ref, index):
        return [(ref[index + (0, s)], ref[index + (1, s)]) for s in range(2)]

    def fine_copies(n):
        phase = 4 * n
        return [
            remote(phase, 0, ht_s.at[n], ht_r.at[n]),
            remote(phase, 1, gt_s.at[n], gt_r.at[n]),
            remote(phase, 2, hz_s.at[n], hz_r.at[n]),
            remote(phase, 3, gz_s.at[n], gz_r.at[n]),
            remote(phase, 4, hx_s.at[n], hx_r.at[n]),
            remote(phase, 5, gx_s.at[n], gx_r.at[n]),
        ]

    def fine_send(vec, n):
        copies = fine_copies(n)

        def send_x():
            ahead = None
            behind = None
            for t in range(4):
                here = lane // 32 == t
                half = project(vec, t, 2, -1)
                back = times_dagger(links, 2, t, project(vec, t, 2, 1))
                store_half(gx, (t,), back)
                half = each(half, lambda a: pltpu.roll(a, 32 * t, 2) if t else a)
                back = each(back, lambda a: pltpu.roll(a, (32 * t + 32) % 128, 2) if t < 3 else a)
                ahead = half if t == 0 else both(half, ahead, lambda a, b: jnp.where(here, a, b))
                behind = back if t == 0 else both(back, behind, lambda a, b: jnp.where(here, a, b))
            store_half(hx_s, (n,), ahead)
            store_half(gx_s, (n,), behind)

        def step_z(t, carry):
            half = project(vec, t, 1, -1)
            for s in range(2):
                for q in range(2):
                    hz_s[n, q, s, :, t : t + 1, :] = half[s][q][:, 0:1, :]
            back = times_dagger(links, 1, t, project(vec, t, 1, 1))
            store_half(gz, (t,), back)
            store_half(gz_s, (n, t), each(back, lambda a: a[:, 7:8, :]))
            return carry

        store_half(ht_s, (n,), project(vec, 0, 0, -1))
        store_half(gt_s, (n,), times_dagger(links, 0, 3, project(vec, 3, 0, 1)))
        if n == 0:
            pl.semaphore_wait(barrier, 6)
        copies[0].start()
        copies[1].start()
        if n == 0:
            loads[9].wait()
            for i in (7, 8, 6, 2, 3, 5, 4):
                loads[i].start()
        send_x()
        copies[4].start()
        copies[5].start()
        if n == 0:
            loads[10].wait()
        for t in range(4):
            step_z(t, 0)
        copies[2].start()
        copies[3].start()
        return copies

    def fine_inner(start, vec):
        def step(t, carry):
            half = project(vec, t, 3, -1)
            half = each(half, lambda a: jnp.where(place_y == 31, sign_y * pltpu.roll(a, 31, 2), pltpu.roll(a, 127, 2)))
            total = add_hop(None, times_link(links, 3, t, half), 3, -1)
            back = times_dagger(links, 3, t, project(vec, t, 3, 1))
            back = each(back, lambda a: jnp.where(place_y == 0, sign_y * pltpu.roll(a, 97, 2), pltpu.roll(a, 1, 2)))
            total = add_hop(total, back, 3, 1)
            for chirality in range(2):
                out_re = [None, None]
                out_im = [None, None]
                for column in range(6):
                    spin, colour = 2 * chirality + column // 3, column % 3
                    vr = vec[0, spin, colour, t][None]
                    vi = vec[1, spin, colour, t][None]
                    for s in range(2):
                        mr = clover[chirality, 0, 3 * s : 3 * s + 3, column, t]
                        mi = clover[chirality, 1, 3 * s : 3 * s + 3, column, t]
                        re = mr * vr - mi * vi
                        im = mr * vi + mi * vr
                        out_re[s] = re if column == 0 else out_re[s] + re
                        out_im[s] = im if column == 0 else out_im[s] + im
                for s in range(2):
                    spin = 2 * chirality + s
                    vr, vi = spin_of(vec, spin, t)
                    part[0, spin, :, t] = start[0, spin, :, t] - MASS_TERM * vr - out_re[s] + 0.5 * total[spin][0]
                    part[1, spin, :, t] = start[1, spin, :, t] - MASS_TERM * vi - out_im[s] + 0.5 * total[spin][1]
            return carry

        def add_part(t, total):
            for spin in range(4):
                for q in range(2):
                    part[q, spin, :, t] = part[q, spin, :, t] + 0.5 * total[spin][q]

        def step_zx(t, carry):
            half = each(project(vec, t, 1, -1), lambda a: jnp.where(row == 7, 0.0, pltpu.roll(a, 7, 1)))
            total = add_hop(None, times_link(links, 1, t, half), 1, -1)
            back = each(load_half(gz, (t,)), lambda a: jnp.where(row == 0, 0.0, pltpu.roll(a, 1, 1)))
            total = add_hop(total, back, 1, 1)
            half = each(project(vec, t, 2, -1), lambda a: jnp.where(lane >= 96, 0.0, pltpu.roll(a, 96, 2)))
            total = add_hop(total, times_link(links, 2, t, half), 2, -1)
            back = each(load_half(gx, (t,)), lambda a: jnp.where(lane < 32, 0.0, pltpu.roll(a, 32, 2)))
            add_part(t, add_hop(total, back, 2, 1))
            return carry

        def step_t(t, carry):
            add_part(t, add_hop(None, times_link(links, 0, t, project(vec, t + 1, 0, -1)), 0, -1))
            add_part(t + 1, add_hop(None, times_dagger(links, 0, t, project(vec, t, 0, 1)), 0, 1))
            return carry

        lax.fori_loop(0, 4, step, 0)
        lax.fori_loop(0, 4, step_zx, 0)
        lax.fori_loop(0, 3, step_t, 0)

    def prepare_edges():
        lane9 = lax.broadcasted_iota(jnp.int32, (3, 3, 8, 128), 3)
        for p in range(2):
            gathered = None
            for t in range(4):
                block = links[2, p, :, :, t]
                if t < 3:
                    block = pltpu.roll(block, (32 * t + 32) % 128, 3)
                gathered = block if t == 0 else jnp.where(lane9 // 32 == t, block, gathered)
                uz[p, :, :, t : t + 1, :] = links[1, p, :, :, t, 7:8, :]
            ux[p] = gathered

    def fine_outer(vec, n, out, keep):
        def scaled(half, sign):
            factor = 0.5 * sign
            return each(half, lambda a: a * factor)

        ahead_t = times_link(links, 0, 3, scaled(load_half(ht_r, (n,)), top[0]))
        behind_t = scaled(load_half(gt_r, (n,)), bottom[0])
        ahead_x = times_packed(ux, scaled(load_half(hx_r, (n,)), top[2]))
        behind_x = scaled(load_half(gx_r, (n,)), bottom[2])
        store_half(rz, (), times_packed(uz, scaled(load_half(hz_r, (n,)), top[1])))
        for t in range(4):
            half = each(ahead_x, lambda a: jnp.where(lane >= 96, pltpu.roll(a, 96 - 32 * t, 2) if t < 3 else a, 0.0))
            total = add_hop(None, half, 2, -1)
            half = each(behind_x, lambda a: jnp.where(lane < 32, pltpu.roll(a, 128 - 32 * t, 2) if t else a, 0.0))
            total = add_hop(total, half, 2, 1)
            half = [(rz[0, s, :, t : t + 1, :], rz[1, s, :, t : t + 1, :]) for s in range(2)]
            total = add_hop(total, each(half, lambda a: jnp.where(row == 7, a, 0.0)), 1, -1)
            half = scaled(load_half(gz_r, (n, t)), bottom[1])
            total = add_hop(total, each(half, lambda a: jnp.where(row == 0, a, 0.0)), 1, 1)
            if t == 3:
                total = add_hop(total, ahead_t, 0, -1)
            if t == 0:
                total = add_hop(total, behind_t, 0, 1)
            for spin in range(4):
                for q in range(2):
                    value = part[q, spin, :, t] + total[spin][q]
                    out[q, spin, :, t] = value
                    if keep:
                        for z in range(2):
                            for colour in range(3):
                                wide[z, q, 3 * spin + colour, 4 * t : 4 * t + 4] = value[colour, 4 * z : 4 * z + 4]

    loads[0].wait()
    loads[1].wait()
    first = fine_send(iterate, 0)
    for i in (7, 8, 6, 2):
        loads[i].wait()
    loads[3].wait()
    top = [sign_of(axis, me[axis] == size[axis] - 1) for axis in range(3)]
    bottom = [sign_of(axis, me[axis] == 0) for axis in range(3)]
    sign_y = bc_ref[3].astype(F32)
    prepare_edges()
    fine_inner(source, iterate)

    loads[5].wait()
    rrow[...] = jnp.zeros_like(rrow)
    for copy in first:
        copy.wait_recv()
    fine_outer(iterate, 0, res, True)

    row2 = lax.broadcasted_iota(jnp.int32, (8, 128), 0)
    lane2 = lax.broadcasted_iota(jnp.int32, (8, 128), 1)
    spread = (lane2 % 32 // 4 == row2).astype(F32)

    def round_step(s, carry):
        for z in range(2):
            re = wide[z, 0, s].astype(jnp.bfloat16)
            im = wide[z, 1, s].astype(jnp.bfloat16)
            field[z, 0, s] = re
            field[z, 1, s] = im
            field[z, 2, s] = -re
        return carry

    for s in range(12):
        round_step(s, 0)

    def running(total, a, b):
        product = a.astype(F32) * b.astype(F32)
        return product if total is None else total + product

    for z in range(2):
        slot = slot_ref[z]

        def restrict_step(i, carry):
            for j in range(12):
                first_v = 2 * j
                totals = [[None, None], [None, None]]
                for s in range(12):
                    for u in range(2):
                        nr = null_b[slot, 0, first_v + u, s]
                        ni = null_b[slot, 1, first_v + u, s]
                        totals[u][0] = running(totals[u][0], nr, field[z, 0, s])
                        totals[u][1] = running(totals[u][1], nr, field[z, 1, s])
                        totals[u][0] = running(totals[u][0], ni, field[z, 1, s])
                        totals[u][1] = running(totals[u][1], ni, field[z, 2, s])
                for u in range(2):
                    for q in range(2):
                        rrow[pl.ds(64 * q + 32 * z + first_v + u, 1)] = jnp.sum(totals[u][q], axis=0, keepdims=True)
            return carry

        restrict_step(0, 0)

    rhs = lax.dot_general(
        spread, rrow[...], (((1,), (1,)), ((), ())), precision=HIGHEST, preferred_element_type=F32
    )
    w = RELAX_WEIGHT * rhs
    lower_z = lane2 % 64 < 32
    lower_p = lane2 < 64
    parity = jnp.where(lower_p, 1.0, -1.0)

    def accumulate(sums, k, vector):
        blocks = packed[k]
        re = blocks * (vector * parity)[None]
        im = blocks * pltpu.roll(vector, 64, 1)[None]
        return (re, im) if sums is None else (sums[0] + re, sums[1] + im)

    def folded(low, high, distance):
        lanes = lax.broadcasted_iota(jnp.int32, low.shape, low.ndim - 1)
        clear = lanes // distance % 2 == 0
        axis = low.ndim - 1
        return jnp.where(clear, low, pltpu.roll(high, distance, axis)) + jnp.where(
            clear, pltpu.roll(low, 128 - distance, axis), high
        )

    gap = jnp.zeros((8, 8), F32)

    def pack_step(k, carry):
        for i in range(NV):
            pieces = []
            for p in range(2):
                for z in range(2):
                    pieces += [coarse_b[k, p, i, z], gap]
            packed[k, i] = jnp.concatenate(pieces, axis=-1)
        return carry

    sent = []
    for iteration in range(3):
        wbuf[iteration] = w
        phase = 1 + iteration
        copies = [
            remote(phase, d, wbuf.at[iteration], c_halo.at[iteration, d]) for d in range(6)
        ]
        for copy in copies:
            copy.start()
        sent += copies
        if iteration == 0:
            loads[4].wait()
            lax.fori_loop(0, 9, pack_step, 0)
        sums = accumulate(None, 0, w)
        sums = accumulate(sums, 7, pltpu.roll(w, 7, 0))
        sums = accumulate(sums, 8, pltpu.roll(w, 1, 0))
        copies[2].wait_recv()
        copies[3].wait_recv()
        ahead = jnp.where(lower_z, pltpu.roll(w, 96, 1), pltpu.roll(c_halo[iteration, 2], 32, 1))
        sums = accumulate(sums, 3, ahead)
        behind = jnp.where(lower_z, pltpu.roll(c_halo[iteration, 3], 96, 1), pltpu.roll(w, 32, 1))
        sums = accumulate(sums, 4, behind)
        for k, d in ((1, 0), (2, 1), (5, 4), (6, 5)):
            copies[d].wait_recv()
            sums = accumulate(sums, k, c_halo[iteration, d])
        wide_p = lax.broadcasted_iota(jnp.int32, (NV, 8, 128), 2) < 64
        folds = jnp.where(wide_p, sums[0], sums[1]) + pltpu.roll(jnp.where(wide_p, sums[1], sums[0]), 64, 2)
        middle = folds[8:16]
        bit = lax.broadcasted_iota(jnp.int32, (8, 8, 128), 2) // 16 % 2 == 0
        middle = jnp.where(bit, middle + pltpu.roll(middle, 112, 2), 0.0)
        folds = folded(folded(folds[0:8], folds[16:24], 16), middle, 8)
        folds = folded(folds[0:4], folds[4:8], 4)
        folds = folded(folds[0:2], folds[2:4], 2)
        total = folded(folds[0], folds[1], 1)
        w = w + RELAX_WEIGHT * (rhs - (2.0 * w + total))

    coef[...] = jnp.dot(
        jnp.transpose(w.astype(jnp.bfloat16).astype(F32)), spread, preferred_element_type=F32
    )
    def tile_step(v, carry):
        for z in range(2):
            re = jnp.broadcast_to(coef[pl.ds(32 * z + v, 1)], (16, 128))
            im = jnp.broadcast_to(coef[pl.ds(64 + 32 * z + v, 1)], (16, 128))
            for kind, value in enumerate((re, im, -im)):
                tile[z, kind, v] = value.astype(jnp.bfloat16)
        return carry

    for v in range(NV):
        tile_step(v, 0)

    for z in range(2):
        slot = slot_ref[z]

        def prolong_step(i, carry):
            totals = [[None, None], [None, None]]
            for v in range(NV):
                for p in range(2):
                    for u in range(2):
                        null = null_b[slot, p, v, 2 * i + u]
                        for q in range(2):
                            kind = ((0, 2), (1, 0))[q][p]
                            totals[u][q] = running(totals[u][q], null, tile[z, kind, v])
            for u in range(2):
                s = 2 * i + u
                spin, colour = s // 3, s % 3
                for q in range(2):
                    for t in range(4):
                        corr[q, spin, colour, t, 4 * z : 4 * z + 4] = totals[u][q][4 * t : 4 * t + 4]
            return carry

        def prolong_pair(i, carry):
            prolong_step(2 * i, carry)
            return prolong_step(2 * i + 1, carry)

        for i in range(3):
            prolong_pair(i, 0)

    second = fine_send(corr, 1)

    def add_step(t, carry):
        out_x[:, :, :, t] = iterate[:, :, :, t] + corr[:, :, :, t]
        return carry

    lax.fori_loop(0, 4, add_step, 0)
    fine_inner(res, corr)
    for copy in second:
        copy.wait_recv()
    fine_outer(corr, 1, out_r, False)
    for copy in first + sent + second:
        copy.wait_send()


def copy_out(x_v, r_v, x_h, r_h, sem):
    copies = [pltpu.make_async_copy(x_v, x_h, sem.at[0]), pltpu.make_async_copy(r_v, r_h, sem.at[1])]
    for copy in copies:
        copy.start()
    for copy in copies:
        copy.wait()


def per_device(source, iterate, gauge_links, clover, bc_sign, null_store, block_slot, coarse_links):
    null = null_store.reshape((2, 2, NV, 12, 16, 128))
    coarse = jnp.transpose(coarse_links, (0, 1, 2, 4, 5, 6, 7, 3)).reshape((9, 2, NV, 2, 8, NV))
    slots = block_slot.reshape((2,))
    spinor = pltpu.VMEM((2, 4, 3, 4, 8, 128), F32)
    anywhere = pl.BlockSpec(memory_space=pl.ANY)
    half = (2, 2, 3, 8, 128)
    vmem = lambda *shape: pltpu.VMEM(shape, F32)
    held = pl.pallas_call(
        kernel,
        out_shape=(spinor, spinor),
        in_specs=[anywhere] * 8,
        out_specs=(pl.BlockSpec(memory_space=pltpu.VMEM),) * 2,
        scratch_shapes=[
            vmem(*spinor.shape), vmem(*spinor.shape), vmem(4, 2, 3, 3, 4, 8, 128),
            vmem(2, 2, 6, 6, 4, 8, 128), pltpu.VMEM((2, 2, NV, 12, 16, 128), jnp.bfloat16),
            vmem(9, 2, NV, 2, 8, NV), vmem(9, NV, 8, 128),
            vmem(2, *half), vmem(2, *half), vmem(2, *half), vmem(2, *half),
            vmem(2, 3, 3, 8, 128), vmem(2, 3, 3, 4, 128), vmem(2, 2, 3, 4, 128), vmem(4, *half), vmem(4, *half),
            vmem(2, 2, 2, 3, 4, 128), vmem(2, 4, 2, 2, 3, 1, 128), vmem(2, *half), vmem(2, *half),
            vmem(2, 2, 2, 3, 4, 128), vmem(2, 4, 2, 2, 3, 1, 128), vmem(2, *half), vmem(2, *half),
            vmem(*spinor.shape), vmem(*spinor.shape), vmem(*spinor.shape), vmem(2, 2, 12, 16, 128),
            pltpu.VMEM((2, 3, 12, 16, 128), jnp.bfloat16), vmem(128, 128), vmem(128, 128),
            pltpu.VMEM((2, 3, NV, 16, 128), jnp.bfloat16), vmem(3, 8, 128), vmem(3, 6, 8, 128),
            pltpu.SMEM((4,), jnp.int32), pltpu.SMEM((2,), jnp.int32), pltpu.SemaphoreType.DMA((11,)), pltpu.SemaphoreType.DMA((5, 6)),
            pltpu.SemaphoreType.DMA((5, 6)),
        ],
        compiler_params=pltpu.CompilerParams(
            collective_id=0, has_side_effects=True, vmem_limit_bytes=56 * 1024 * 1024
        ),
    )(source, iterate, gauge_links, clover, null, coarse, bc_sign, slots)
    held = [pltpu.with_memory_space_constraint(x, pltpu.VMEM) for x in held]
    final = jax.ShapeDtypeStruct(spinor.shape, F32)
    return pl.pallas_call(
        copy_out,
        out_shape=(final, final),
        in_specs=[pl.BlockSpec(memory_space=pltpu.VMEM)] * 2,
        out_specs=(anywhere, anywhere),
        scratch_shapes=[pltpu.SemaphoreType.DMA((2,))],
    )(*held)


def solution(mesh):
    spinor = P(None, None, None, "ta", "gz", "xy")
    matrix = P(None, None, None, None, "ta", "gz", "xy")
    column = P("ta", "gz", "xy", None, None, None, None, None, None)
    placed = (
        spinor, spinor, matrix, matrix, P(), column, P("ta", "gz", "xy"),
        P(None, None, None, None, "ta", "gz", "xy", None),
    )
    return jax.shard_map(
        per_device, mesh=mesh, in_specs=placed, out_specs=(spinor, spinor), check_vma=False
    )
```
